32 devices in a mesh: dp: 2 (over x), ep: 16 (over z, y, core).
Axes of the slice: x: 2, y: 2, z: 4, core: 2. Of those that a mesh axis runs over, the one named last changes fastest.
Arguments:
- x_tokens: bfloat16 [16384, 2048], P(('dp', 'ep')), parts along dimension 0
- slot_expert: int32 [80], replicated
- w1_slots: bfloat16 [80, 2048, 1408], P('ep')
- w3_slots: bfloat16 [80, 2048, 1408], P('ep')
- w2_slots: bfloat16 [80, 1408, 2048], P('ep')
- assign: int32 [16384, 6], P(('dp', 'ep')), parts along dimension 0
- w_router: bfloat16 [2048, 64], replicated
- w1_shared: bfloat16 [2048, 2816], replicated
- w3_shared: bfloat16 [2048, 2816], replicated
- w2_shared: bfloat16 [2816, 2048], replicated
Outputs:
- output: bfloat16 [16384, 2048], P(('dp', 'ep')), parts along dimension 0
There are 2 independent parts. The reference program is written for one: setup_inputs(seed, part) draws one part's arguments, and reference() takes and returns one part's arrays. A program takes and returns all parts, laid end to end along the dimension named above; an argument that names none is the same for every part.
All inputs are finite; a program needn't handle non-finite values.
Results may differ from the reference program's by a relative error of at most 0.00158.
Values are sent between devices in bfloat16 or wider.
A program may use at most 1 GiB of HBM per device.

```python
import jax
import jax.numpy as jnp
from jax import lax

DIM_MODEL = 2048
FF_EXPERT = 1408
FF_SHARED = 2816
NUM_EXPERTS = 64
TOP_K = 6
NUM_SLOTS = 80
GROUP_SIZE = 16
TOK_DEV = 512

TOKENS = TOK_DEV * GROUP_SIZE
CAP_ROWS = max(4, (3 * TOK_DEV * TOP_K) // NUM_SLOTS)
SEG_ROWS = min(TOKENS, GROUP_SIZE * CAP_ROWS)
ROUTE_SCALE = 2.5


def draw_routing(key_shared, key_part):
    key_rank, key_place = jax.random.split(key_shared, 2)
    rank_expert = jax.random.permutation(key_rank, NUM_EXPERTS).astype(jnp.int32)
    base_of_slot = jax.random.permutation(key_place, NUM_SLOTS).astype(jnp.int32)
    slot_expert = rank_expert[base_of_slot % NUM_EXPERTS]
    slot_of_base = jnp.argsort(base_of_slot).astype(jnp.int32)
    key_noise, key_coin, key_pick = jax.random.split(key_part, 3)
    rank_ids = jnp.arange(NUM_EXPERTS, dtype=jnp.int32)
    rank_bias = (2 * TOP_K * 4096) // (NUM_EXPERTS * (rank_ids + 1))
    noise_int = jax.random.randint(key_noise, (TOKENS, NUM_EXPERTS), 0, 4096, dtype=jnp.int32)
    token_ids = jnp.arange(TOKENS, dtype=jnp.int32)
    forced = token_ids < CAP_ROWS
    force_bonus = jnp.where(forced[:, None] & (rank_ids[None, :] == 0), 16384, 0)
    rank_score = (noise_int + rank_bias[None, :] + force_bonus) * NUM_EXPERTS + rank_ids[None, :]
    chosen_rank = lax.top_k(rank_score, TOP_K)[1].astype(jnp.int32)
    copies = (NUM_SLOTS - 1 - chosen_rank) // NUM_EXPERTS + 1
    coin_flip = jax.random.randint(key_coin, (TOKENS, TOP_K), 0, 2, dtype=jnp.int32)
    pick_copy = jax.random.randint(key_pick, (TOKENS, TOP_K), 0, 65536, dtype=jnp.int32) % copies
    keep_first = (coin_flip == 0) | (forced[:, None] & (chosen_rank == 0))
    copy_index = jnp.where(keep_first, 0, pick_copy)
    slot_pick = slot_of_base[chosen_rank + copy_index * NUM_EXPERTS]
    device_of = (token_ids // TOK_DEV)[:, None]
    group_key = (device_of * NUM_SLOTS + slot_pick).reshape(-1)
    sort_order = jnp.argsort(group_key, stable=True)
    sorted_key = group_key[sort_order]
    first_pos = jnp.searchsorted(sorted_key, sorted_key, side='left').astype(jnp.int32)
    rank_sorted = jnp.arange(TOKENS * TOP_K, dtype=jnp.int32) - first_pos
    rank_flat = jnp.zeros((TOKENS * TOP_K,), jnp.int32).at[sort_order].set(rank_sorted)
    assign = jnp.where(rank_flat < CAP_ROWS, slot_pick.reshape(-1), -1).reshape(TOKENS, TOP_K)
    return slot_expert, assign.astype(jnp.int32)


def setup_inputs(seed: int = 0, part: int = 0) -> dict:
    weight_keys = jax.random.split(jax.random.key(seed), 8)
    part_key = jax.random.fold_in(jax.random.key(seed + 1), part)
    key_tokens, key_route = jax.random.split(part_key, 2)
    slot_expert, assign = draw_routing(weight_keys[0], key_route)
    x_tokens = jax.random.normal(key_tokens, (TOKENS, DIM_MODEL), jnp.float32)
    w1_experts = jax.random.normal(weight_keys[1], (NUM_EXPERTS, DIM_MODEL, FF_EXPERT), jnp.float32) * DIM_MODEL ** -0.5
    w3_experts = jax.random.normal(weight_keys[2], (NUM_EXPERTS, DIM_MODEL, FF_EXPERT), jnp.float32) * DIM_MODEL ** -0.5
    w2_experts = jax.random.normal(weight_keys[3], (NUM_EXPERTS, FF_EXPERT, DIM_MODEL), jnp.float32) * FF_EXPERT ** -0.5
    w_router = jax.random.normal(weight_keys[4], (DIM_MODEL, NUM_EXPERTS), jnp.float32) * DIM_MODEL ** -0.5
    w1_shared = jax.random.normal(weight_keys[5], (DIM_MODEL, FF_SHARED), jnp.float32) * DIM_MODEL ** -0.5
    w3_shared = jax.random.normal(weight_keys[6], (DIM_MODEL, FF_SHARED), jnp.float32) * DIM_MODEL ** -0.5
    w2_shared = jax.random.normal(weight_keys[7], (FF_SHARED, DIM_MODEL), jnp.float32) * FF_SHARED ** -0.5
    return {
        'x_tokens': x_tokens.astype(jnp.bfloat16),
        'slot_expert': slot_expert,
        'w1_slots': w1_experts.astype(jnp.bfloat16)[slot_expert],
        'w3_slots': w3_experts.astype(jnp.bfloat16)[slot_expert],
        'w2_slots': w2_experts.astype(jnp.bfloat16)[slot_expert],
        'assign': assign,
        'w_router': w_router.astype(jnp.bfloat16),
        'w1_shared': w1_shared.astype(jnp.bfloat16),
        'w3_shared': w3_shared.astype(jnp.bfloat16),
        'w2_shared': w2_shared.astype(jnp.bfloat16),
    }


def gate_weights(x_tokens, assign, slot_expert, w_router):
    logits = jnp.dot(x_tokens, w_router, preferred_element_type=jnp.float32)
    gate_prob = jax.nn.sigmoid(logits)
    is_kept = assign >= 0
    chosen = slot_expert[jnp.maximum(assign, 0)]
    picked = jnp.where(is_kept, jnp.take_along_axis(gate_prob, chosen, axis=1), 0.0)
    gate_total = jnp.sum(picked, axis=1, keepdims=True)
    return ROUTE_SCALE * picked / jnp.maximum(gate_total, 1e-30), is_kept


def shared_expert(x_tokens, w1_shared, w3_shared, w2_shared):
    h_gate = jnp.dot(x_tokens, w1_shared, preferred_element_type=jnp.float32)
    h_up = jnp.dot(x_tokens, w3_shared, preferred_element_type=jnp.float32)
    mid_act = (jax.nn.silu(h_gate) * h_up).astype(jnp.bfloat16)
    return jnp.dot(mid_act, w2_shared, preferred_element_type=jnp.float32)


def reference(x_tokens, slot_expert, w1_slots, w3_slots, w2_slots, assign, w_router, w1_shared, w3_shared, w2_shared):
    route_weight, is_kept = gate_weights(x_tokens, assign, slot_expert, w_router)
    shared_out = shared_expert(x_tokens, w1_shared, w3_shared, w2_shared)
    flat_slot = jnp.where(is_kept, assign, NUM_SLOTS).reshape(-1)
    sort_order = jnp.argsort(flat_slot, stable=True)
    sorted_slot = flat_slot[sort_order]
    slot_ids = jnp.arange(NUM_SLOTS, dtype=jnp.int32)
    seg_start = jnp.searchsorted(sorted_slot, slot_ids, side='left').astype(jnp.int32)
    seg_end = jnp.searchsorted(sorted_slot, slot_ids, side='right').astype(jnp.int32)
    token_list = jnp.concatenate([(sort_order // TOP_K).astype(jnp.int32), jnp.zeros((SEG_ROWS,), jnp.int32)])
    weight_list = jnp.concatenate([route_weight.reshape(-1)[sort_order], jnp.zeros((SEG_ROWS,), route_weight.dtype)])
    row_offsets = jnp.arange(SEG_ROWS, dtype=jnp.int32)

    def slot_step(acc_rows, slot_id):
        seg_begin = seg_start[slot_id]
        row_ids = lax.dynamic_slice(token_list, (seg_begin,), (SEG_ROWS,))
        row_weight = lax.dynamic_slice(weight_list, (seg_begin,), (SEG_ROWS,))
        row_weight = jnp.where(row_offsets < seg_end[slot_id] - seg_begin, row_weight, 0.0)
        x_rows = x_tokens[row_ids]
        h_gate = jnp.dot(x_rows, w1_slots[slot_id], preferred_element_type=jnp.float32)
        h_up = jnp.dot(x_rows, w3_slots[slot_id], preferred_element_type=jnp.float32)
        mid_act = (jax.nn.silu(h_gate) * h_up).astype(jnp.bfloat16)
        out_rows = jnp.dot(mid_act, w2_slots[slot_id], preferred_element_type=jnp.float32).astype(jnp.bfloat16)
        acc_rows = acc_rows.at[row_ids].add(row_weight[:, None] * out_rows.astype(jnp.float32))
        return acc_rows, None

    routed = lax.scan(slot_step, jnp.zeros((TOKENS, DIM_MODEL), jnp.float32), slot_ids)[0]
    return (shared_out + routed).astype(jnp.bfloat16)
```

```python
import jax
import jax.numpy as jnp
from jax import lax
from jax.experimental import pallas as pl
from jax.experimental.pallas import tpu as pltpu
from jax.sharding import PartitionSpec as P

ROUTE_SCALE = 2.5
TM = 256
WIN = 128
ALIGN = 16


def gate_weights(x_tokens, assign, slot_expert, w_router):
    logits = jnp.dot(x_tokens, w_router, preferred_element_type=jnp.float32)
    gate_prob = jax.nn.sigmoid(logits)
    is_kept = assign >= 0
    chosen = jnp.take(slot_expert, jnp.maximum(assign, 0))
    hit = chosen[:, :, None] == jnp.arange(gate_prob.shape[1], dtype=jnp.int32)
    picked = jnp.sum(jnp.where(hit, gate_prob[:, None, :], 0.0), axis=2)
    picked = jnp.where(is_kept, picked, 0.0)
    gate_total = jnp.sum(picked, axis=1, keepdims=True)
    return ROUTE_SCALE * picked / jnp.maximum(gate_total, 1e-30)


def shared_expert(x_tokens, w1_shared, w3_shared, w2_shared):
    h_gate = jnp.dot(x_tokens, w1_shared, preferred_element_type=jnp.float32)
    h_up = jnp.dot(x_tokens, w3_shared, preferred_element_type=jnp.float32)
    mid_act = (jax.nn.silu(h_gate) * h_up).astype(jnp.bfloat16)
    return jnp.dot(mid_act, w2_shared, preferred_element_type=jnp.float32)


def dispatch(x_all, rank_rows, off, cpad, tail, max_rows):
    blocks, _, tok = rank_rows.shape
    slots = tail.shape[0]
    dim = x_all.shape[1]

    def kernel(off_ref, cpad_ref, tail_ref, rank_ref, x_ref, out_ref, stage, zeros, sem, zsem):
        b = pl.program_id(0)
        buf = lax.rem(b, 2)

        def copy16(i, src_row, dst_row):
            return pltpu.make_async_copy(
                stage.at[i, pl.ds(pl.multiple_of(src_row, ALIGN), ALIGN), :],
                out_ref.at[pl.ds(pl.multiple_of(dst_row, ALIGN), ALIGN), :],
                sem.at[i],
            )

        def drain(step, i):
            total = cpad_ref[step * slots]
            for s in range(1, slots):
                total = total + cpad_ref[step * slots + s]

            def body(_, c):
                copy16(i, 0, 0).wait()
                return c

            lax.fori_loop(0, lax.div(total, ALIGN), body, 0)

        @pl.when(b >= 2)
        def _():
            drain(b - 2, buf)

        rows = lax.broadcasted_iota(jnp.int32, (WIN, tok), 0)
        sel = [(rows == rank_ref[0, s : s + 1, :]).astype(jnp.float32).astype(jnp.bfloat16) for s in range(slots)]
        win = jnp.dot(jnp.concatenate(sel, axis=0), x_ref[...], preferred_element_type=jnp.float32)
        stage[buf] = win.astype(jnp.bfloat16)
        for s in range(slots):
            start = off_ref[b * slots + s]

            def body(c, carry):
                copy16(buf, s * WIN + c * ALIGN, start + c * ALIGN).start()
                return carry

            lax.fori_loop(0, lax.div(cpad_ref[b * slots + s], ALIGN), body, 0)

        @pl.when(b == blocks - 1)
        def _():
            zeros[...] = jnp.zeros_like(zeros)

            def zcopy(row):
                return pltpu.make_async_copy(zeros, out_ref.at[pl.ds(pl.multiple_of(row, ALIGN), ALIGN), :], zsem)

            for wait in (False, True):
                for s in range(slots):
                    first = off_ref[b * slots + s] + cpad_ref[b * slots + s]

                    def body(c, carry):
                        d = zcopy(first + c * ALIGN)
                        d.wait() if wait else d.start()
                        return carry

                    lax.fori_loop(0, lax.div(tail_ref[s] - first, ALIGN), body, 0)
            drain(b - 1, 1 - buf)
            drain(b, buf)

    return pl.pallas_call(
        kernel,
        grid_spec=pltpu.PrefetchScalarGridSpec(
            num_scalar_prefetch=3,
            grid=(blocks,),
            in_specs=[
                pl.BlockSpec((1, rank_rows.shape[1], tok), lambda b, *_: (b, 0, 0)),
                pl.BlockSpec((tok, dim), lambda b, *_: (b, 0)),
            ],
            out_specs=pl.BlockSpec(memory_space=pl.ANY),
            scratch_shapes=[
                pltpu.VMEM((2, slots * WIN, dim), jnp.bfloat16),
                pltpu.VMEM((ALIGN, dim), jnp.bfloat16),
                pltpu.SemaphoreType.DMA((2,)),
                pltpu.SemaphoreType.DMA,
            ],
        ),
        out_shape=jax.ShapeDtypeStruct((max_rows, dim), jnp.bfloat16),
        compiler_params=pltpu.CompilerParams(vmem_limit_bytes=48 * 2**20),
        name="dispatch",
    )(off, cpad, tail, rank_rows, x_all)


def expert_mlp(x_rows, w1, w3, w2, tile_slot, num_tiles):
    dim, ff = w1.shape[1:]

    def kernel(slot_ref, tiles_ref, x_ref, w1_ref, w3_ref, w2_ref, o_ref):
        @pl.when(pl.program_id(0) < tiles_ref[0])
        def _():
            x = x_ref[...]
            gate = jnp.dot(x, w1_ref[0], preferred_element_type=jnp.float32)
            up = jnp.dot(x, w3_ref[0], preferred_element_type=jnp.float32)
            mid = (jax.nn.silu(gate) * up).astype(jnp.bfloat16)
            o_ref[...] = jnp.dot(mid, w2_ref[0], preferred_element_type=jnp.float32).astype(jnp.bfloat16)

    def row_block(i, slot, tiles):
        return jnp.minimum(i, tiles[0] - 1), 0

    return pl.pallas_call(
        kernel,
        grid_spec=pltpu.PrefetchScalarGridSpec(
            num_scalar_prefetch=2,
            grid=(x_rows.shape[0] // TM,),
            in_specs=[
                pl.BlockSpec((TM, dim), row_block),
                pl.BlockSpec((1, dim, ff), lambda i, slot, tiles: (slot[i], 0, 0)),
                pl.BlockSpec((1, dim, ff), lambda i, slot, tiles: (slot[i], 0, 0)),
                pl.BlockSpec((1, ff, dim), lambda i, slot, tiles: (slot[i], 0, 0)),
            ],
            out_specs=pl.BlockSpec((TM, dim), row_block),
        ),
        out_shape=jax.ShapeDtypeStruct(x_rows.shape, jnp.bfloat16),
        compiler_params=pltpu.CompilerParams(vmem_limit_bytes=60 * 2**20),
        name="expert_mlp",
    )(tile_slot, num_tiles.reshape(1), x_rows, w1, w3, w2)


def combine(o_rows, rank_cols, w_cols, win_start):
    blocks, tok, slots = rank_cols.shape
    dim = o_rows.shape[1]

    def kernel(start_ref, rank_ref, w_ref, o_ref, out_ref, wins, sem):
        b = pl.program_id(0)
        buf = lax.rem(b, 2)

        def fetch(step, i):
            return [
                pltpu.make_async_copy(
                    o_ref.at[pl.ds(pl.multiple_of(start_ref[step * slots + s], ALIGN), WIN), :],
                    wins.at[i, pl.ds(s * WIN, WIN), :],
                    sem.at[i, s],
                )
                for s in range(slots)
            ]

        @pl.when(b == 0)
        def _():
            for c in fetch(b, buf):
                c.start()

        @pl.when(b + 1 < blocks)
        def _():
            for c in fetch(b + 1, 1 - buf):
                c.start()

        lanes = lax.broadcasted_iota(jnp.int32, (tok, WIN), 1)
        a = jnp.concatenate(
            [jnp.where(lanes == rank_ref[0, :, s : s + 1], w_ref[0, :, s : s + 1], 0.0) for s in range(slots)], axis=1
        )
        hi = a.astype(jnp.bfloat16)
        rest = a - hi.astype(jnp.float32)
        mid = rest.astype(jnp.bfloat16)
        low = (rest - mid.astype(jnp.float32)).astype(jnp.bfloat16)
        for c in fetch(b, buf):
            c.wait()
        o = wins[buf]
        acc = jnp.dot(hi, o, preferred_element_type=jnp.float32)
        acc += jnp.dot(mid, o, preferred_element_type=jnp.float32)
        acc += jnp.dot(low, o, preferred_element_type=jnp.float32)
        out_ref[...] = acc

    return pl.pallas_call(
        kernel,
        grid_spec=pltpu.PrefetchScalarGridSpec(
            num_scalar_prefetch=1,
            grid=(blocks,),
            in_specs=[
                pl.BlockSpec((1, tok, slots), lambda b, *_: (b, 0, 0)),
                pl.BlockSpec((1, tok, slots), lambda b, *_: (b, 0, 0)),
                pl.BlockSpec(memory_space=pl.ANY),
            ],
            out_specs=pl.BlockSpec((tok, dim), lambda b, *_: (b, 0)),
            scratch_shapes=[
                pltpu.VMEM((2, slots * WIN, dim), jnp.bfloat16),
                pltpu.SemaphoreType.DMA((2, slots)),
            ],
        ),
        out_shape=jax.ShapeDtypeStruct((blocks * tok, dim), jnp.float32),
        compiler_params=pltpu.CompilerParams(vmem_limit_bytes=56 * 2**20),
        name="combine",
    )(win_start, rank_cols, w_cols, o_rows)


def routing_plan(assign_all, weight_all, first_slot, slots):
    blocks, tok, _ = assign_all.shape
    hit = (assign_all - first_slot)[..., None] == jnp.arange(slots, dtype=jnp.int32)
    member = jnp.any(hit, axis=2)
    weight = jnp.sum(jnp.where(hit, weight_all[..., None], 0.0), axis=2)
    upto = (jnp.arange(tok)[:, None] >= jnp.arange(tok)[None, :]).astype(jnp.bfloat16)
    order = jnp.einsum('pq,bqs->bps', upto, member.astype(jnp.bfloat16), preferred_element_type=jnp.float32)
    order = order.astype(jnp.int32)
    count = order[:, -1, :]
    rank = jnp.where(member, order - 1, -4 * WIN)
    cpad = (count + ALIGN - 1) // ALIGN * ALIGN
    inside = jnp.cumsum(cpad, axis=0) - cpad
    tiles = (jnp.sum(cpad, axis=0) + TM - 1) // TM
    tile_end = jnp.cumsum(tiles)
    off = ((tile_end - tiles) * TM)[None, :] + inside
    return rank, weight, cpad, off, tile_end


def solution(mesh):
    group_size = mesh.shape['ep']

    def device_step(x_tokens, slot_expert, w1_slots, w3_slots, w2_slots, assign, w_router, w1_shared, w3_shared, w2_shared):
        tok, dim = x_tokens.shape
        top_k = assign.shape[1]
        slots = w1_slots.shape[0]
        me = lax.axis_index('ep')
        max_tiles = slots * (group_size * WIN // TM)
        weight = gate_weights(x_tokens, assign, slot_expert, w_router)
        meta = lax.all_gather(jnp.concatenate([assign.astype(jnp.float32), weight], axis=1), 'ep')
        x_all = lax.all_gather(x_tokens, 'ep', tiled=True)
        shared_out = shared_expert(x_tokens, w1_shared, w3_shared, w2_shared)
        rank, w_all, cpad, off, tile_end = routing_plan(
            meta[..., :top_k].astype(jnp.int32), meta[..., top_k:], me * slots, slots
        )
        num_tiles = jnp.maximum(tile_end[-1], 1)
        tile_ids = jnp.arange(max_tiles, dtype=jnp.int32)
        tile_slot = jnp.sum((jnp.minimum(tile_ids, num_tiles - 1)[:, None] >= tile_end[None, :-1]).astype(jnp.int32), axis=1)
        tail = (tile_end * TM).at[-1].set(num_tiles * TM)
        rank_rows = jnp.pad(jnp.transpose(rank, (0, 2, 1)), ((0, 0), (0, 8 - slots), (0, 0)), constant_values=-1)
        x_rows = dispatch(x_all, rank_rows, off.reshape(-1), cpad.reshape(-1), tail, max_tiles * TM)
        o_rows = expert_mlp(x_rows, w1_slots, w3_slots, w2_slots, tile_slot, num_tiles)
        win_start = jnp.minimum(off, num_tiles * TM - WIN)
        partial = combine(o_rows, rank + (off - win_start)[:, None, :], w_all, win_start.reshape(-1))
        routed = lax.psum_scatter(partial, 'ep', scatter_dimension=0, tiled=True)
        return (shared_out + routed).astype(jnp.bfloat16)

    token_spec = P(('dp', 'ep'), None)
    slot_spec = P('ep', None, None)
    return jax.shard_map(device_step, mesh=mesh, in_specs=(token_spec, P(), slot_spec, slot_spec, slot_spec, token_spec, P(), P(), P(), P()), out_specs=token_spec, check_vma=False)
```

```python
import jax
import jax.numpy as jnp
from jax import lax
from jax.experimental import pallas as pl
from jax.experimental.pallas import tpu as pltpu
from jax.sharding import PartitionSpec as P

ROUTE_SCALE = 2.5
TM = 256
WIN = 128
ALIGN = 16
CAP = 384
PIECE = 512
MESH = pl.DeviceIdType.MESH


def gate_weights(x_tokens, assign, slot_expert, w_router):
    num_experts, num_slots = w_router.shape[1], slot_expert.shape[0]
    pick = (jnp.arange(num_experts, dtype=jnp.int32)[:, None] == slot_expert[None, :]).astype(w_router.dtype)
    w_slot = jnp.dot(w_router, pick)
    gate_prob = jax.nn.sigmoid(jnp.dot(x_tokens, w_slot, preferred_element_type=jnp.float32))
    hit = assign[:, :, None] == jnp.arange(num_slots, dtype=jnp.int32)
    picked = jnp.sum(jnp.where(hit, gate_prob[:, None, :], 0.0), axis=2)
    gate_total = jnp.sum(picked, axis=1, keepdims=True)
    return ROUTE_SCALE * picked / jnp.maximum(gate_total, 1e-30)


def shared_expert(x_tokens, w1_shared, w3_shared, w2_shared):
    h_gate = jnp.dot(x_tokens, w1_shared, preferred_element_type=jnp.float32)
    h_up = jnp.dot(x_tokens, w3_shared, preferred_element_type=jnp.float32)
    mid_act = (jax.nn.silu(h_gate) * h_up).astype(jnp.bfloat16)
    return jnp.dot(mid_act, w2_shared, preferred_element_type=jnp.float32)


def dispatch(x_all, rank_rows, off, cpad, tail, max_rows):
    blocks, _, tok = rank_rows.shape
    slots = tail.shape[0]
    dim = x_all.shape[1]

    def kernel(off_ref, cpad_ref, tail_ref, rank_ref, x_ref, out_ref, stage, zeros, sem, zsem):
        b = pl.program_id(0)
        buf = lax.rem(b, 2)

        def copy16(i, src_row, dst_row):
            return pltpu.make_async_copy(
                stage.at[i, pl.ds(pl.multiple_of(src_row, ALIGN), ALIGN), :],
                out_ref.at[pl.ds(pl.multiple_of(dst_row, ALIGN), ALIGN), :],
                sem.at[i],
            )

        def drain(step, i):
            total = cpad_ref[step * slots]
            for s in range(1, slots):
                total = total + cpad_ref[step * slots + s]

            def body(_, c):
                copy16(i, 0, 0).wait()
                return c

            lax.fori_loop(0, lax.div(total, ALIGN), body, 0)

        @pl.when(b >= 2)
        def _():
            drain(b - 2, buf)

        rows = lax.broadcasted_iota(jnp.int32, (WIN, tok), 0)
        sel = [(rows == rank_ref[0, s : s + 1, :]).astype(jnp.float32).astype(jnp.bfloat16) for s in range(slots)]
        win = jnp.dot(jnp.concatenate(sel, axis=0), x_ref[...], preferred_element_type=jnp.float32)
        stage[buf] = win.astype(jnp.bfloat16)
        for s in range(slots):
            start = off_ref[b * slots + s]

            def body(c, carry):
                copy16(buf, s * WIN + c * ALIGN, start + c * ALIGN).start()
                return carry

            lax.fori_loop(0, lax.div(cpad_ref[b * slots + s], ALIGN), body, 0)

        @pl.when(b == blocks - 1)
        def _():
            zeros[...] = jnp.zeros_like(zeros)

            def zcopy(row):
                return pltpu.make_async_copy(zeros, out_ref.at[pl.ds(pl.multiple_of(row, ALIGN), ALIGN), :], zsem)

            for wait in (False, True):
                for s in range(slots):
                    first = off_ref[b * slots + s] + cpad_ref[b * slots + s]

                    def body(c, carry):
                        d = zcopy(first + c * ALIGN)
                        d.wait() if wait else d.start()
                        return carry

                    lax.fori_loop(0, lax.div(tail_ref[s] - first, ALIGN), body, 0)
            drain(b - 1, 1 - buf)
            drain(b, buf)

    return pl.pallas_call(
        kernel,
        grid_spec=pltpu.PrefetchScalarGridSpec(
            num_scalar_prefetch=3,
            grid=(blocks,),
            in_specs=[
                pl.BlockSpec((1, rank_rows.shape[1], tok), lambda b, *_: (b, 0, 0)),
                pl.BlockSpec((tok, dim), lambda b, *_: (b, 0)),
            ],
            out_specs=pl.BlockSpec(memory_space=pl.ANY),
            scratch_shapes=[
                pltpu.VMEM((2, slots * WIN, dim), jnp.bfloat16),
                pltpu.VMEM((ALIGN, dim), jnp.bfloat16),
                pltpu.SemaphoreType.DMA((2,)),
                pltpu.SemaphoreType.DMA,
            ],
        ),
        out_shape=jax.ShapeDtypeStruct((max_rows, dim), jnp.bfloat16),
        compiler_params=pltpu.CompilerParams(vmem_limit_bytes=48 * 2**20),
        name="dispatch",
    )(off, cpad, tail, rank_rows, x_all)


def expert_mlp(x_rows, w1, w3, w2, tile_slot, num_tiles, chunk_dst, chunk_count, used, out_rows):
    dim, ff = w1.shape[1:]
    tiles_max = x_rows.shape[0] // TM
    chunks = TM // ALIGN
    parts = out_rows // CAP

    def kernel(slot_ref, tiles_ref, dst_ref, count_ref, used_ref, x_ref, w1_ref, w3_ref, w2_ref, o_ref, stage, zeros, sem, zsem):
        i = pl.program_id(0)
        buf = lax.rem(i, 2)
        tiles = tiles_ref[0]

        def copy16(k, c, row):
            return pltpu.make_async_copy(
                stage.at[k, pl.ds(pl.multiple_of(c * ALIGN, ALIGN), ALIGN), :],
                o_ref.at[pl.ds(pl.multiple_of(row * ALIGN, ALIGN), ALIGN), :],
                sem.at[k],
            )

        def drain(step, k):
            def body(_, carry):
                copy16(k, 0, 0).wait()
                return carry

            lax.fori_loop(0, count_ref[step], body, 0)

        def zero_fill(wait):
            def part(p, carry):
                def body(c, carry):
                    d = pltpu.make_async_copy(
                        zeros, o_ref.at[pl.ds(pl.multiple_of(p * CAP + c * ALIGN, ALIGN), ALIGN), :], zsem
                    )
                    d.wait() if wait else d.start()
                    return carry

                return lax.fori_loop(used_ref[p], CAP // ALIGN, body, carry)

            lax.fori_loop(0, parts, part, 0)

        @pl.when(i == 0)
        def _():
            zeros[...] = jnp.zeros_like(zeros)
            zero_fill(False)

        @pl.when(i < tiles)
        def _():
            x = x_ref[...]
            gate = jnp.dot(x, w1_ref[0], preferred_element_type=jnp.float32)
            up = jnp.dot(x, w3_ref[0], preferred_element_type=jnp.float32)
            mid = (jax.nn.silu(gate) * up).astype(jnp.bfloat16)
            out = jnp.dot(mid, w2_ref[0], preferred_element_type=jnp.float32).astype(jnp.bfloat16)

            @pl.when(i >= 2)
            def _():
                drain(i - 2, buf)

            stage[buf] = out

            def body(c, carry):
                copy16(buf, c, dst_ref[i * chunks + c]).start()
                return carry

            lax.fori_loop(0, count_ref[i], body, 0)

        @pl.when(i == tiles_max - 1)
        def _():
            last = tiles - 1

            @pl.when(tiles >= 2)
            def _():
                drain(last - 1, lax.rem(last + 1, 2))

            drain(last, lax.rem(last, 2))
            zero_fill(True)

    def row_block(i, slot, tiles, *_):
        return jnp.minimum(i, tiles[0] - 1), 0

    def slot_block(i, slot, *_):
        return slot[i], 0, 0

    return pl.pallas_call(
        kernel,
        grid_spec=pltpu.PrefetchScalarGridSpec(
            num_scalar_prefetch=5,
            grid=(tiles_max,),
            in_specs=[
                pl.BlockSpec((TM, dim), row_block),
                pl.BlockSpec((1, dim, ff), slot_block),
                pl.BlockSpec((1, dim, ff), slot_block),
                pl.BlockSpec((1, ff, dim), slot_block),
            ],
            out_specs=pl.BlockSpec(memory_space=pl.ANY),
            scratch_shapes=[
                pltpu.VMEM((2, TM, dim), jnp.bfloat16),
                pltpu.VMEM((ALIGN, dim), jnp.bfloat16),
                pltpu.SemaphoreType.DMA((2,)),
                pltpu.SemaphoreType.DMA,
            ],
        ),
        out_shape=jax.ShapeDtypeStruct((out_rows, dim), jnp.bfloat16),
        compiler_params=pltpu.CompilerParams(vmem_limit_bytes=60 * 2**20),
        name="expert_mlp",
    )(tile_slot, num_tiles.reshape(1), chunk_dst, chunk_count, used, x_rows, w1, w3, w2)


def exchange(o_send, plan, turn):
    dim = o_send.shape[1]
    layers, tok, _ = plan.shape
    pieces = dim // PIECE
    units = layers * pieces
    rows = 4 * CAP
    top_k = 6

    def kernel(send_ref, plan_ref, out_ref, recv, zbuf, stage, sel, raw_send, raw_recv, own_sem, z_send, z_recv, out_sem):
        me = lax.axis_index('ep')
        z = me // 4
        q = lax.rem(me, 4)

        def home_of(i):
            low = jnp.where(z == 0, 3 - i, jnp.where(i == 0, 3, jnp.where(i == 1, 0, jnp.where(i == 2, 2, 1))))
            r = 3 - z
            high = jnp.where(r == 0, i, jnp.where(i == 0, 0, jnp.where(i == 1, 3, jnp.where(i == 2, 1, 2))))
            return jnp.where(z < 2, low, high)

        barrier = pltpu.get_barrier_semaphore()
        for d in range(1, 4):
            peer = z * 4 + lax.rem(q + d, 4)
            pl.semaphore_signal(barrier, inc=1, device_id={'ep': peer}, device_id_type=MESH)

        @pl.when(z > 0)
        def _():
            pl.semaphore_signal(barrier, inc=1, device_id={'ep': me - 4}, device_id_type=MESH)

        @pl.when(z < 3)
        def _():
            pl.semaphore_signal(barrier, inc=1, device_id={'ep': me + 4}, device_id_type=MESH)

        pl.semaphore_wait(barrier, 3 + jnp.where(z > 0, 1, 0) + jnp.where(z < 3, 1, 0))

        def block(dst_q, u):
            home, p = home_of(u // pieces), lax.rem(u, pieces)
            row = ((turn * 4 + dst_q) * 4 + home) * CAP
            return send_ref.at[pl.ds(pl.multiple_of(row, ALIGN), CAP), pl.ds(pl.multiple_of(p * PIECE, PIECE), PIECE)]

        def raw(d, u):
            dst_q = lax.rem(q + d, 4)
            return pltpu.make_async_remote_copy(
                src_ref=block(dst_q, u),
                dst_ref=recv.at[u, pl.ds(pl.multiple_of(q * CAP, CAP), CAP), :],
                send_sem=raw_send.at[d - 1, u],
                recv_sem=raw_recv.at[d - 1, u],
                device_id={'ep': z * 4 + dst_q},
                device_id_type=MESH,
            )

        def own(u):
            return pltpu.make_async_copy(
                block(q, u), recv.at[u, pl.ds(pl.multiple_of(q * CAP, CAP), CAP), :], own_sem.at[u]
            )

        def start_raw(u, carry):
            for d in range(1, 4):
                raw(d, u).start()
            own(u).start()
            return carry

        lax.fori_loop(0, units, start_raw, 0)

        def up(slot, u):
            return pltpu.make_async_remote_copy(
                src_ref=stage.at[lax.rem(u, 4)],
                dst_ref=zbuf.at[slot, lax.rem(u, pieces)],
                send_sem=z_send.at[lax.rem(u, 4)],
                recv_sem=z_recv.at[slot, lax.rem(u, pieces)],
                device_id={'ep': me + 4},
                device_id_type=MESH,
            )

        def down(slot, u):
            return pltpu.make_async_remote_copy(
                src_ref=stage.at[lax.rem(u, 4)],
                dst_ref=zbuf.at[slot, lax.rem(u, pieces)],
                send_sem=z_send.at[lax.rem(u, 4)],
                recv_sem=z_recv.at[slot, lax.rem(u, pieces)],
                device_id={'ep': me - 4},
                device_id_type=MESH,
            )

        def finish(u):
            p = lax.rem(u, pieces)
            return pltpu.make_async_copy(
                stage.at[lax.rem(u, 4)], out_ref.at[:, pl.ds(pl.multiple_of(p * PIECE, PIECE), PIECE)], out_sem.at[p]
            )

        def unit(u, carry):
            home, p = home_of(u // pieces), lax.rem(u, pieces)
            k = lax.rem(u, 4)

            @pl.when(p == 0)
            def _():
                lanes = lax.broadcasted_iota(jnp.int32, (tok, CAP), 1).astype(jnp.float32)
                mine = plan_ref[home]
                for src in range(4):
                    a = jnp.zeros((tok, CAP), jnp.float32)
                    for c in range(top_k):
                        a = jnp.where(lanes == mine[:, c : c + 1] - float(src * CAP), mine[:, 8 + c : 9 + c], a)
                    hi = a.astype(jnp.bfloat16)
                    rest = a - hi.astype(jnp.float32)
                    mid = rest.astype(jnp.bfloat16)
                    sel[0, :, src * CAP : (src + 1) * CAP] = hi
                    sel[1, :, src * CAP : (src + 1) * CAP] = mid
                    sel[2, :, src * CAP : (src + 1) * CAP] = (rest - mid.astype(jnp.float32)).astype(jnp.bfloat16)

            for d in range(1, 4):
                raw(d, u).wait()
            own(u).wait()
            o = recv[u]
            acc = jnp.dot(sel[0], o, preferred_element_type=jnp.float32)
            acc += jnp.dot(sel[1], o, preferred_element_type=jnp.float32)
            acc += jnp.dot(sel[2], o, preferred_element_type=jnp.float32)

            @pl.when(u >= 4)
            def _():
                up(0, u - 4).wait_send()

            stage[k] = acc

            @pl.when(((home < z) & (z < 3)) | ((home >= z) & (z > 0)))
            def _():
                up(home, u).wait_recv()
                stage[k] += zbuf[home, p]

            @pl.when((home == z) & (z < 3))
            def _():
                up(4, u).wait_recv()
                stage[k] += zbuf[4, p]

            @pl.when(home > z)
            def _():
                up(home, u).start()

            @pl.when(home < z)
            def _():
                down(jnp.where(home == z - 1, 4, home), u).start()

            @pl.when(home == z)
            def _():
                finish(u).start()

            return carry

        lax.fori_loop(0, units, unit, 0)
        for u in range(units - pieces, units):
            finish(u).wait()

    return pl.pallas_call(
        kernel,
        out_shape=jax.ShapeDtypeStruct((tok, dim), jnp.float32),
        in_specs=[pl.BlockSpec(memory_space=pl.ANY), pl.BlockSpec(memory_space=pltpu.VMEM)],
        out_specs=pl.BlockSpec(memory_space=pl.ANY),
        scratch_shapes=[
            pltpu.VMEM((units, rows, PIECE), jnp.bfloat16),
            pltpu.VMEM((5, pieces, tok, PIECE), jnp.float32),
            pltpu.VMEM((4, tok, PIECE), jnp.float32),
            pltpu.VMEM((3, tok, rows), jnp.bfloat16),
            pltpu.SemaphoreType.DMA((3, units)),
            pltpu.SemaphoreType.DMA((3, units)),
            pltpu.SemaphoreType.DMA((units,)),
            pltpu.SemaphoreType.DMA((4,)),
            pltpu.SemaphoreType.DMA((5, pieces)),
            pltpu.SemaphoreType.DMA((pieces,)),
        ],
        compiler_params=pltpu.CompilerParams(
            collective_id=1 + turn, has_side_effects=True, vmem_limit_bytes=66_000_000
        ),
        name="exchange",
    )(o_send, plan)


def running_count(assign_all, num_slots):
    tok = assign_all.shape[1]
    member = jnp.any(assign_all[..., None] == jnp.arange(num_slots, dtype=jnp.int32), axis=2)
    upto = (jnp.arange(tok)[:, None] >= jnp.arange(tok)[None, :]).astype(jnp.bfloat16)
    order = jnp.einsum('pq,bqs->bps', upto, member.astype(jnp.bfloat16), preferred_element_type=jnp.float32)
    return member, order.astype(jnp.int32)


def solution(mesh):
    group_size = mesh.shape['ep']

    def device_step(x_tokens, slot_expert, w1_slots, w3_slots, w2_slots, assign, w_router, w1_shared, w3_shared, w2_shared):
        tok, dim = x_tokens.shape
        top_k = assign.shape[1]
        slots = w1_slots.shape[0]
        num_slots = slots * group_size
        me = lax.axis_index('ep')
        my_z, my_q = me // 4, me % 4
        max_tiles = slots * (group_size * WIN // TM)
        chunks = TM // ALIGN
        weight = gate_weights(x_tokens, assign, slot_expert, w_router)
        x_all = lax.all_gather(x_tokens, 'ep', tiled=True)
        meta = lax.all_gather(jnp.concatenate([assign.astype(jnp.float32), weight], axis=1), 'ep')
        assign_all = meta[..., :top_k].astype(jnp.int32)
        w_all = meta[..., top_k:]
        shared_out = shared_expert(x_tokens, w1_shared, w3_shared, w2_shared)

        member, order = running_count(assign_all, num_slots)
        count = order[:, -1, :]
        cpad = (count + ALIGN - 1) // ALIGN * ALIGN
        by_dev = cpad.reshape(group_size, group_size, slots)
        crowded = jnp.max(jnp.sum(by_dev, axis=2)) > CAP
        crowded = lax.pmax(crowded.astype(jnp.int32), ('dp', 'ep')) > 0
        split = CAP // WIN
        in_turn = jnp.where(crowded & (jnp.arange(slots) >= split), 1, 0)
        before = jnp.cumsum(by_dev, axis=2) - by_dev
        place = before - jnp.where(in_turn == 1, before[:, :, split : split + 1], 0)
        turn_of = jnp.broadcast_to(in_turn, (group_size, slots)).reshape(num_slots)

        mine = lax.dynamic_slice_in_dim(cpad, me * slots, slots, axis=1)
        my_order = lax.dynamic_slice_in_dim(order, me * slots, slots, axis=2)
        my_member = lax.dynamic_slice_in_dim(member, me * slots, slots, axis=2)
        my_place = lax.dynamic_slice_in_dim(place, me, 1, axis=1)[:, 0]
        tiles = (jnp.sum(mine, axis=0) + TM - 1) // TM
        tile_end = jnp.cumsum(tiles)
        inside = jnp.cumsum(mine, axis=0) - mine
        off = ((tile_end - tiles) * TM)[None, :] + inside
        num_tiles = jnp.maximum(tile_end[-1], 1)
        tile_ids = jnp.arange(max_tiles, dtype=jnp.int32)
        tile_slot = jnp.sum((jnp.minimum(tile_ids, num_tiles - 1)[:, None] >= tile_end[None, :-1]).astype(jnp.int32), axis=1)
        tail = jnp.concatenate([tile_end[:-1], num_tiles[None]]) * TM
        rank = jnp.where(my_member, my_order - 1, -1)
        rank_rows = jnp.pad(jnp.transpose(rank, (0, 2, 1)), ((0, 0), (0, 8 - slots), (0, 0)), constant_values=-1)

        home = jnp.arange(group_size, dtype=jnp.int32)
        base = (in_turn[None, :] * 16 + ((home % 4) * 4 + home // 4)[:, None]) * CAP + my_place
        row0 = jnp.arange(max_tiles * chunks, dtype=jnp.int32) * ALIGN
        lo, hi = off.reshape(-1), (off + mine).reshape(-1)
        inside_group = (row0[:, None] >= lo[None, :]) & (row0[:, None] < hi[None, :])
        chunk_dst = jnp.sum(jnp.where(inside_group, (base - off).reshape(-1)[None, :] + row0[:, None], 0), axis=1) // ALIGN
        chunk_count = jnp.sum(inside_group.reshape(max_tiles, chunks, -1).astype(jnp.int32), axis=(1, 2))
        filled = jnp.stack(
            [jnp.sum(jnp.where(in_turn == 0, mine, 0), axis=1), jnp.where(crowded, jnp.sum(jnp.where(in_turn == 1, mine, 0), axis=1), CAP)]
        )
        used = jnp.transpose(filled.reshape(2, 4, 4), (0, 2, 1)).reshape(-1) // ALIGN

        sum_order = lax.dynamic_slice_in_dim(order.reshape(4, 4, tok, num_slots), my_q, 1, axis=1)[:, 0]
        sum_place = lax.dynamic_slice_in_dim(place.reshape(4, 4, num_slots), my_q, 1, axis=1)[:, 0]
        sum_assign = lax.dynamic_slice_in_dim(assign_all.reshape(4, 4, tok, top_k), my_q, 1, axis=1)[:, 0]
        sum_weight = lax.dynamic_slice_in_dim(w_all.reshape(4, 4, tok, top_k), my_q, 1, axis=1)[:, 0]
        layer_slots = 4 * slots
        slot_ids = jnp.arange(num_slots, dtype=jnp.int32)
        arrives = jnp.where(
            slot_ids // layer_slots == my_z, (slot_ids // slots) % 4 * CAP + sum_place, -(2**20)
        )[:, None, :] + sum_order - 1
        hit = sum_assign[..., None] == slot_ids

        def plan_of(turn):
            col = jnp.sum(jnp.where(hit & (turn_of == turn), arrives[:, :, None, :] + 1, 0), axis=3) - 1
            pad = ((0, 0), (0, 0), (0, 8 - top_k))
            return jnp.concatenate(
                [jnp.pad(col.astype(jnp.float32), pad, constant_values=-1.0), jnp.pad(sum_weight, pad)], axis=2
            )

        x_all, shared_out = lax.optimization_barrier((x_all, shared_out))
        x_rows = dispatch(x_all, rank_rows, off.reshape(-1), mine.reshape(-1), tail, max_tiles * TM)
        o_send = expert_mlp(
            x_rows, w1_slots, w3_slots, w2_slots, tile_slot, num_tiles, chunk_dst, chunk_count, used, 32 * CAP
        )
        routed = exchange(o_send, plan_of(0), 0)
        routed = lax.cond(
            crowded, lambda r, o, p: r + exchange(o, p, 1), lambda r, o, p: r, routed, o_send, plan_of(1)
        )
        return (shared_out + routed).astype(jnp.bfloat16)

    token_spec = P(('dp', 'ep'), None)
    slot_spec = P('ep', None, None)
    return jax.shard_map(device_step, mesh=mesh, in_specs=(token_spec, P(), slot_spec, slot_spec, slot_spec, token_spec, P(), P(), P(), P()), out_specs=token_spec, check_vma=False)
```

```python
import jax
import jax.numpy as jnp
from jax import lax
from jax.experimental import pallas as pl
from jax.experimental.pallas import tpu as pltpu
from jax.sharding import PartitionSpec as P

ROUTE_SCALE = 2.5
TM = 256
WIN = 128
ALIGN = 8
CHUNKS = (256, 256)
CAP = 384
PIECE = 512
MESH = pl.DeviceIdType.MESH


def gate_weights(x_tokens, assign, slot_expert, w_router):
    num_experts, num_slots = w_router.shape[1], slot_expert.shape[0]
    pick = (jnp.arange(num_experts, dtype=jnp.int32)[:, None] == slot_expert[None, :]).astype(w_router.dtype)
    w_slot = jnp.dot(w_router, pick)
    gate_prob = jax.nn.sigmoid(jnp.dot(x_tokens, w_slot, preferred_element_type=jnp.float32))
    hit = assign[:, :, None] == jnp.arange(num_slots, dtype=jnp.int32)
    picked = jnp.sum(jnp.where(hit, gate_prob[:, None, :], 0.0), axis=2)
    gate_total = jnp.sum(picked, axis=1, keepdims=True)
    return ROUTE_SCALE * picked / jnp.maximum(gate_total, 1e-30)


def shared_expert(x_tokens, w1_shared, w3_shared, w2_shared):
    h_gate = jnp.dot(x_tokens, w1_shared, preferred_element_type=jnp.float32)
    h_up = jnp.dot(x_tokens, w3_shared, preferred_element_type=jnp.float32)
    mid_act = (jax.nn.silu(h_gate) * h_up).astype(jnp.bfloat16)
    return jnp.dot(mid_act, w2_shared, preferred_element_type=jnp.float32)


def dispatch(x_all, rank_rows, off, cpad, tail, max_rows):
    blocks, _, tok = rank_rows.shape
    slots = tail.shape[0]
    dim = x_all.shape[1]

    def kernel(off_ref, cpad_ref, tail_ref, rank_ref, x_ref, out_ref, stage, zeros, sem, zsem):
        b = pl.program_id(0)
        buf = lax.rem(b, 2)

        def copy16(i, src_row, dst_row):
            return pltpu.make_async_copy(
                stage.at[i, pl.ds(pl.multiple_of(src_row, ALIGN), ALIGN), :],
                out_ref.at[pl.ds(pl.multiple_of(dst_row, ALIGN), ALIGN), :],
                sem.at[i],
            )

        def drain(step, i):
            total = cpad_ref[step * slots]
            for s in range(1, slots):
                total = total + cpad_ref[step * slots + s]

            def body(_, c):
                copy16(i, 0, 0).wait()
                return c

            lax.fori_loop(0, lax.div(total, ALIGN), body, 0)

        @pl.when(b >= 2)
        def _():
            drain(b - 2, buf)

        rows = lax.broadcasted_iota(jnp.int32, (WIN, tok), 0)
        sel = [(rows == rank_ref[0, s : s + 1, :]).astype(jnp.float32).astype(jnp.bfloat16) for s in range(slots)]
        win = jnp.dot(jnp.concatenate(sel, axis=0), x_ref[...], preferred_element_type=jnp.float32)
        stage[buf] = win.astype(jnp.bfloat16)
        for s in range(slots):
            start = off_ref[b * slots + s]

            def body(c, carry):
                copy16(buf, s * WIN + c * ALIGN, start + c * ALIGN).start()
                return carry

            lax.fori_loop(0, lax.div(cpad_ref[b * slots + s], ALIGN), body, 0)

        @pl.when(b == blocks - 1)
        def _():
            zeros[...] = jnp.zeros_like(zeros)

            def zcopy(row):
                return pltpu.make_async_copy(zeros, out_ref.at[pl.ds(pl.multiple_of(row, ALIGN), ALIGN), :], zsem)

            for wait in (False, True):
                for s in range(slots):
                    first = off_ref[b * slots + s] + cpad_ref[b * slots + s]

                    def body(c, carry):
                        d = zcopy(first + c * ALIGN)
                        d.wait() if wait else d.start()
                        return carry

                    lax.fori_loop(0, lax.div(tail_ref[s] - first, ALIGN), body, 0)
            drain(b - 1, 1 - buf)
            drain(b, buf)

    return pl.pallas_call(
        kernel,
        grid_spec=pltpu.PrefetchScalarGridSpec(
            num_scalar_prefetch=3,
            grid=(blocks,),
            in_specs=[
                pl.BlockSpec((1, rank_rows.shape[1], tok), lambda b, *_: (b, 0, 0)),
                pl.BlockSpec((tok, dim), lambda b, *_: (b, 0)),
            ],
            out_specs=pl.BlockSpec(memory_space=pl.ANY),
            scratch_shapes=[
                pltpu.VMEM((2, slots * WIN, dim), jnp.bfloat16),
                pltpu.VMEM((ALIGN, dim), jnp.bfloat16),
                pltpu.SemaphoreType.DMA((2,)),
                pltpu.SemaphoreType.DMA,
            ],
        ),
        out_shape=jax.ShapeDtypeStruct((max_rows, dim), jnp.bfloat16),
        compiler_params=pltpu.CompilerParams(vmem_limit_bytes=48 * 2**20),
        name="dispatch",
    )(off, cpad, tail, rank_rows, x_all)


def expert_mlp(x_rows, w1, w3, w2, tile_slot, num_tiles, chunk_dst, chunk_count, used, out):
    dim, ff = w1.shape[1:]
    first = isinstance(out, int)
    out_rows = out if first else out.shape[0]
    tiles_max = x_rows.shape[0] // TM
    chunks = TM // ALIGN
    parts = out_rows // CAP

    def kernel(slot_ref, tiles_ref, dst_ref, count_ref, used_ref, x_ref, w1_ref, w3_ref, w2_ref, *rest):
        o_ref, stage, zeros, sem, zsem = rest[-5:]
        i = pl.program_id(0)
        buf = lax.rem(i, 2)
        tiles = tiles_ref[0]

        def copy16(k, c, row):
            return pltpu.make_async_copy(
                stage.at[k, pl.ds(pl.multiple_of(c * ALIGN, ALIGN), ALIGN), :],
                o_ref.at[pl.ds(pl.multiple_of(row * ALIGN, ALIGN), ALIGN), :],
                sem.at[k],
            )

        def drain(step, k):
            def body(_, carry):
                copy16(k, 0, 0).wait()
                return carry

            lax.fori_loop(0, count_ref[step], body, 0)

        def zero_fill(wait):
            def part(p, carry):
                def body(c, carry):
                    d = pltpu.make_async_copy(
                        zeros, o_ref.at[pl.ds(pl.multiple_of(p * CAP + c * ALIGN, ALIGN), ALIGN), :], zsem
                    )
                    d.wait() if wait else d.start()
                    return carry

                return lax.fori_loop(used_ref[p], CAP // ALIGN, body, carry)

            lax.fori_loop(0, parts, part, 0)

        if first:

            @pl.when(i == 0)
            def _():
                zeros[...] = jnp.zeros_like(zeros)
                zero_fill(False)

        @pl.when(i < tiles)
        def _():
            x = x_ref[...]
            gate = jnp.dot(x, w1_ref[0], preferred_element_type=jnp.float32)
            up = jnp.dot(x, w3_ref[0], preferred_element_type=jnp.float32)
            mid = (jax.nn.silu(gate) * up).astype(jnp.bfloat16)
            out = jnp.dot(mid, w2_ref[0], preferred_element_type=jnp.float32).astype(jnp.bfloat16)

            @pl.when(i >= 2)
            def _():
                drain(i - 2, buf)

            stage[buf] = out

            def body(c, carry):
                copy16(buf, c, dst_ref[i * chunks + c]).start()
                return carry

            lax.fori_loop(0, count_ref[i], body, 0)

        @pl.when(i == tiles_max - 1)
        def _():
            last = tiles - 1

            @pl.when(tiles >= 2)
            def _():
                drain(last - 1, lax.rem(last + 1, 2))

            drain(last, lax.rem(last, 2))
            if first:
                zero_fill(True)

    def row_block(i, slot, tiles, *_):
        return jnp.minimum(i, tiles[0] - 1), 0

    def slot_block(i, slot, *_):
        return slot[i], 0, 0

    return pl.pallas_call(
        kernel,
        grid_spec=pltpu.PrefetchScalarGridSpec(
            num_scalar_prefetch=5,
            grid=(tiles_max,),
            in_specs=[
                pl.BlockSpec((TM, dim), row_block),
                pl.BlockSpec((1, dim, ff), slot_block),
                pl.BlockSpec((1, dim, ff), slot_block),
                pl.BlockSpec((1, ff, dim), slot_block),
            ]
            + ([] if first else [pl.BlockSpec(memory_space=pl.ANY)]),
            out_specs=pl.BlockSpec(memory_space=pl.ANY),
            scratch_shapes=[
                pltpu.VMEM((2, TM, dim), jnp.bfloat16),
                pltpu.VMEM((ALIGN, dim), jnp.bfloat16),
                pltpu.SemaphoreType.DMA((2,)),
                pltpu.SemaphoreType.DMA,
            ],
        ),
        out_shape=jax.ShapeDtypeStruct((out_rows, dim), jnp.bfloat16),
        compiler_params=pltpu.CompilerParams(vmem_limit_bytes=60 * 2**20),
        input_output_aliases={} if first else {9: 0},
        name="expert_mlp",
    )(tile_slot, num_tiles.reshape(1), chunk_dst, chunk_count, used, x_rows, w1, w3, w2, *([] if first else [out]))


def exchange(o_send, plan, turn, cap):
    dim = o_send.shape[1]
    layers, tok, _ = plan.shape
    pieces = dim // PIECE
    units = layers * pieces
    rows = 4 * cap
    top_k = 6

    def kernel(send_ref, plan_ref, out_ref, recv, zbuf, stage, sel, raw_send, raw_recv, own_sem, z_send, z_recv, out_sem):
        me = lax.axis_index('ep')
        z = me // 4
        q = lax.rem(me, 4)

        def home_of(i):
            low = jnp.where(z == 0, 3 - i, jnp.where(i == 0, 3, jnp.where(i == 1, 0, jnp.where(i == 2, 2, 1))))
            r = 3 - z
            high = jnp.where(r == 0, i, jnp.where(i == 0, 0, jnp.where(i == 1, 3, jnp.where(i == 2, 1, 2))))
            return jnp.where(z < 2, low, high)

        barrier = pltpu.get_barrier_semaphore()
        for d in range(1, 4):
            peer = z * 4 + lax.rem(q + d, 4)
            pl.semaphore_signal(barrier, inc=1, device_id={'ep': peer}, device_id_type=MESH)

        @pl.when(z > 0)
        def _():
            pl.semaphore_signal(barrier, inc=1, device_id={'ep': me - 4}, device_id_type=MESH)

        @pl.when(z < 3)
        def _():
            pl.semaphore_signal(barrier, inc=1, device_id={'ep': me + 4}, device_id_type=MESH)

        pl.semaphore_wait(barrier, 3 + jnp.where(z > 0, 1, 0) + jnp.where(z < 3, 1, 0))

        def block(dst_q, u):
            home, p = home_of(u // pieces), lax.rem(u, pieces)
            row = ((turn * 4 + dst_q) * 4 + home) * CAP
            return send_ref.at[pl.ds(pl.multiple_of(row, 128), cap), pl.ds(pl.multiple_of(p * PIECE, PIECE), PIECE)]

        def raw(d, u):
            dst_q = lax.rem(q + d, 4)
            return pltpu.make_async_remote_copy(
                src_ref=block(dst_q, u),
                dst_ref=recv.at[u, pl.ds(pl.multiple_of(q * cap, cap), cap), :],
                send_sem=raw_send.at[d - 1, u],
                recv_sem=raw_recv.at[d - 1, u],
                device_id={'ep': z * 4 + dst_q},
                device_id_type=MESH,
            )

        def own(u):
            return pltpu.make_async_copy(
                block(q, u), recv.at[u, pl.ds(pl.multiple_of(q * cap, cap), cap), :], own_sem.at[u]
            )

        def start_raw(u, carry):
            for d in range(1, 4):
                raw(d, u).start()
            own(u).start()
            return carry

        lax.fori_loop(0, units, start_raw, 0)

        def up(slot, u):
            return pltpu.make_async_remote_copy(
                src_ref=stage.at[lax.rem(u, 4)],
                dst_ref=zbuf.at[slot, lax.rem(u, pieces)],
                send_sem=z_send.at[lax.rem(u, 4)],
                recv_sem=z_recv.at[slot, lax.rem(u, pieces)],
                device_id={'ep': me + 4},
                device_id_type=MESH,
            )

        def down(slot, u):
            return pltpu.make_async_remote_copy(
                src_ref=stage.at[lax.rem(u, 4)],
                dst_ref=zbuf.at[slot, lax.rem(u, pieces)],
                send_sem=z_send.at[lax.rem(u, 4)],
                recv_sem=z_recv.at[slot, lax.rem(u, pieces)],
                device_id={'ep': me - 4},
                device_id_type=MESH,
            )

        def finish(u):
            p = lax.rem(u, pieces)
            return pltpu.make_async_copy(
                stage.at[lax.rem(u, 4)], out_ref.at[:, pl.ds(pl.multiple_of(p * PIECE, PIECE), PIECE)], out_sem.at[p]
            )

        def unit(u, carry):
            home, p = home_of(u // pieces), lax.rem(u, pieces)
            k = lax.rem(u, 4)

            @pl.when(p == 0)
            def _():
                lanes = lax.broadcasted_iota(jnp.int32, (tok, cap), 1).astype(jnp.float32)
                mine = plan_ref[home]
                for src in range(4):
                    a = jnp.zeros((tok, cap), jnp.float32)
                    for c in range(top_k):
                        a = jnp.where(lanes == mine[:, c : c + 1] - float(src * cap), mine[:, 8 + c : 9 + c], a)
                    hi = a.astype(jnp.bfloat16)
                    rest = a - hi.astype(jnp.float32)
                    mid = rest.astype(jnp.bfloat16)
                    sel[0, :, src * cap : (src + 1) * cap] = hi
                    sel[1, :, src * cap : (src + 1) * cap] = mid
                    sel[2, :, src * cap : (src + 1) * cap] = (rest - mid.astype(jnp.float32)).astype(jnp.bfloat16)

            for d in range(1, 4):
                raw(d, u).wait()
            own(u).wait()

            @pl.when(u >= 4)
            def _():
                up(0, u - 4).wait_send()

            stage[k] = jnp.dot(sel[0], recv[u], preferred_element_type=jnp.float32)

            def term(j, c):
                stage[k] += jnp.dot(sel[j], recv[u], preferred_element_type=jnp.float32)
                return c

            lax.fori_loop(1, 3, term, 0)

            @pl.when(((home < z) & (z < 3)) | ((home >= z) & (z > 0)))
            def _():
                up(home, u).wait_recv()
                stage[k] += zbuf[home, p]

            @pl.when((home == z) & (z < 3))
            def _():
                up(4, u).wait_recv()
                stage[k] += zbuf[4, p]

            @pl.when(home > z)
            def _():
                up(home, u).start()

            @pl.when(home < z)
            def _():
                down(jnp.where(home == z - 1, 4, home), u).start()

            @pl.when(home == z)
            def _():
                finish(u).start()

            return carry

        lax.fori_loop(0, units, unit, 0)
        for u in range(units - pieces, units):
            finish(u).wait()

    return pl.pallas_call(
        kernel,
        out_shape=jax.ShapeDtypeStruct((tok, dim), jnp.float32),
        in_specs=[pl.BlockSpec(memory_space=pl.ANY), pl.BlockSpec(memory_space=pltpu.VMEM)],
        out_specs=pl.BlockSpec(memory_space=pl.ANY),
        scratch_shapes=[
            pltpu.VMEM((units, rows, PIECE), jnp.bfloat16),
            pltpu.VMEM((5, pieces, tok, PIECE), jnp.float32),
            pltpu.VMEM((4, tok, PIECE), jnp.float32),
            pltpu.VMEM((3, tok, rows), jnp.bfloat16),
            pltpu.SemaphoreType.DMA((3, units)),
            pltpu.SemaphoreType.DMA((3, units)),
            pltpu.SemaphoreType.DMA((units,)),
            pltpu.SemaphoreType.DMA((4,)),
            pltpu.SemaphoreType.DMA((5, pieces)),
            pltpu.SemaphoreType.DMA((pieces,)),
        ],
        compiler_params=pltpu.CompilerParams(
            collective_id=1 + turn, has_side_effects=True, vmem_limit_bytes=66_000_000
        ),
        name="exchange",
    )(o_send, plan)


def running_count(assign_all, num_slots):
    tok = assign_all.shape[1]
    member = jnp.any(assign_all[..., None] == jnp.arange(num_slots, dtype=jnp.int32), axis=2)
    upto = (jnp.arange(tok)[:, None] >= jnp.arange(tok)[None, :]).astype(jnp.bfloat16)
    order = jnp.einsum('pq,bqs->bps', upto, member.astype(jnp.bfloat16), preferred_element_type=jnp.float32)
    return member, order.astype(jnp.int32)


def solution(mesh):
    group_size = mesh.shape['ep']

    def device_step(x_tokens, slot_expert, w1_slots, w3_slots, w2_slots, assign, w_router, w1_shared, w3_shared, w2_shared):
        tok, dim = x_tokens.shape
        top_k = assign.shape[1]
        slots = w1_slots.shape[0]
        num_slots = slots * group_size
        me = lax.axis_index('ep')
        my_z, my_q = me // 4, me % 4
        max_tiles = slots * (group_size * WIN // TM)
        chunks = TM // ALIGN
        weight = gate_weights(x_tokens, assign, slot_expert, w_router)
        ends = [sum(CHUNKS[: c + 1]) for c in range(len(CHUNKS))]
        x_chunks = [lax.all_gather(x_tokens[e - t : e], 'ep', tiled=True) for t, e in zip(CHUNKS, ends)]
        meta = lax.all_gather(jnp.concatenate([assign.astype(jnp.float32), weight], axis=1), ('dp', 'ep'))
        meta = meta.reshape(-1, group_size, tok, 2 * top_k)
        everyone = meta[..., :top_k].astype(jnp.int32)
        my_dp = lax.axis_index('dp')
        assign_all = lax.dynamic_index_in_dim(everyone, my_dp, 0, keepdims=False)
        w_all = lax.dynamic_index_in_dim(meta, my_dp, 0, keepdims=False)[..., top_k:]

        def padded(count):
            return (count + ALIGN - 1) // ALIGN * ALIGN

        member_e = jnp.any(everyone[..., None] == jnp.arange(num_slots, dtype=jnp.int32), axis=3)
        need = sum(
            jnp.sum(padded(jnp.sum(member_e[:, :, e - t : e].astype(jnp.int32), axis=2)).reshape(-1, group_size, slots), axis=2)
            for t, e in zip(CHUNKS, ends)
        )
        crowded = jnp.max(need) > CAP

        member, order = running_count(assign_all, num_slots)
        totals = jnp.stack([order[:, e - 1, :] for e in ends])
        starts = jnp.concatenate([jnp.zeros_like(totals[:1]), totals[:-1]])
        cpad = padded(totals - starts)
        by_dev = jnp.transpose(cpad.reshape(len(CHUNKS), group_size, group_size, slots), (1, 2, 3, 0))
        split = CAP // WIN
        in_turn = jnp.where(crowded & (jnp.arange(slots) >= split), 1, 0)
        flat = by_dev.reshape(group_size, group_size, -1)
        before = (jnp.cumsum(flat, axis=2) - flat).reshape(by_dev.shape)
        place = before - jnp.where(in_turn[:, None] == 1, before[:, :, split : split + 1, :1], 0)
        place = jnp.transpose(place, (3, 0, 1, 2))
        turn_of = jnp.broadcast_to(in_turn, (group_size, slots)).reshape(num_slots)

        my_pad = lax.dynamic_slice_in_dim(cpad, me * slots, slots, axis=2)
        my_start = lax.dynamic_slice_in_dim(starts, me * slots, slots, axis=2)
        my_order = lax.dynamic_slice_in_dim(order, me * slots, slots, axis=2)
        my_member = lax.dynamic_slice_in_dim(member, me * slots, slots, axis=2)
        my_place = lax.dynamic_slice_in_dim(place, me, 1, axis=2)[:, :, 0]
        home = jnp.arange(group_size, dtype=jnp.int32)
        base = (in_turn[None, :] * 16 + ((home % 4) * 4 + home // 4)[:, None]) * CAP
        tile_ids = jnp.arange(max_tiles, dtype=jnp.int32)
        row0 = jnp.arange(max_tiles * chunks, dtype=jnp.int32) * ALIGN

        def chunk_plan(c):
            t, e, mine = CHUNKS[c], ends[c], my_pad[c]
            tiles = (jnp.sum(mine, axis=0) + TM - 1) // TM
            tile_end = jnp.cumsum(tiles)
            off = ((tile_end - tiles) * TM)[None, :] + jnp.cumsum(mine, axis=0) - mine
            num_tiles = jnp.maximum(tile_end[-1], 1)
            tile_slot = jnp.sum((jnp.minimum(tile_ids, num_tiles - 1)[:, None] >= tile_end[None, :-1]).astype(jnp.int32), axis=1)
            tail = jnp.concatenate([tile_end[:-1], num_tiles[None]]) * TM
            rank = jnp.where(my_member[:, e - t : e], my_order[:, e - t : e] - my_start[c][:, None, :] - 1, -1)
            rank_rows = jnp.pad(jnp.transpose(rank, (0, 2, 1)), ((0, 0), (0, 8 - slots), (0, 0)), constant_values=-1)
            lo, hi = off.reshape(-1), (off + mine).reshape(-1)
            inside = (row0[:, None] >= lo[None, :]) & (row0[:, None] < hi[None, :])
            shift = (base + my_place[c] - off).reshape(-1)
            dst = jnp.sum(jnp.where(inside, shift[None, :] + row0[:, None], 0), axis=1) // ALIGN
            count = jnp.sum(inside.reshape(max_tiles, chunks, -1).astype(jnp.int32), axis=(1, 2))
            return (rank_rows, off.reshape(-1), mine.reshape(-1), tail), (tile_slot, num_tiles, dst, count)

        mine = jnp.sum(my_pad, axis=0)
        filled = jnp.stack(
            [jnp.sum(jnp.where(in_turn == 0, mine, 0), axis=1), jnp.where(crowded, jnp.sum(jnp.where(in_turn == 1, mine, 0), axis=1), CAP)]
        )
        used = jnp.transpose(filled.reshape(2, 4, 4), (0, 2, 1)).reshape(-1) // ALIGN

        sum_order = lax.dynamic_slice_in_dim(order.reshape(4, 4, tok, num_slots), my_q, 1, axis=1)[:, 0]
        sum_place = lax.dynamic_slice_in_dim((place.reshape(starts.shape) - starts).reshape(-1, 4, 4, num_slots), my_q, 1, axis=2)[:, :, 0]
        sum_assign = lax.dynamic_slice_in_dim(assign_all.reshape(4, 4, tok, top_k), my_q, 1, axis=1)[:, 0]
        sum_weight = lax.dynamic_slice_in_dim(w_all.reshape(4, 4, tok, top_k), my_q, 1, axis=1)[:, 0]
        slot_ids = jnp.arange(num_slots, dtype=jnp.int32)
        arrives = jnp.where(slot_ids // (4 * slots) == my_z, (slot_ids // slots) % 4 * CAP + sum_place, -(2**20))
        arrives = jnp.concatenate(
            [jnp.broadcast_to(arrives[c][:, None, :], (4, t, num_slots)) for c, t in enumerate(CHUNKS)], axis=1
        ) + sum_order
        hit = sum_assign[..., None] == slot_ids

        def plan_of(turn):
            col = jnp.sum(jnp.where(hit & (turn_of == turn), arrives[:, :, None, :], 0), axis=3) - 1
            pad = ((0, 0), (0, 0), (0, 8 - top_k))
            return jnp.concatenate(
                [jnp.pad(col.astype(jnp.float32), pad, constant_values=-1.0), jnp.pad(sum_weight, pad)], axis=2
            )

        plans = [chunk_plan(c) for c in range(len(CHUNKS))]
        shared_out = shared_expert(x_tokens, w1_shared, w3_shared, w2_shared)
        x_chunks[0], shared_out = lax.optimization_barrier((x_chunks[0], shared_out))
        o_send = 32 * CAP
        for x_part, (rows_plan, tiles_plan) in zip(x_chunks, plans):
            x_rows = dispatch(x_part, *rows_plan, max_tiles * TM)
            o_send = expert_mlp(x_rows, w1_slots, w3_slots, w2_slots, *tiles_plan, used, o_send)
        routed = exchange(o_send, plan_of(0), 0, CAP)
        routed = lax.cond(
            crowded, lambda r, o, p: r + exchange(o, p, 1, CAP), lambda r, o, p: r, routed, o_send, plan_of(1)
        )
        return (shared_out + routed).astype(jnp.bfloat16)

    token_spec = P(('dp', 'ep'), None)
    slot_spec = P('ep', None, None)
    return jax.shard_map(device_step, mesh=mesh, in_specs=(token_spec, P(), slot_spec, slot_spec, slot_spec, token_spec, P(), P(), P(), P()), out_specs=token_spec, check_vma=False)
```

```python
import jax
import jax.numpy as jnp
from jax import lax
from jax.experimental import pallas as pl
from jax.experimental.pallas import tpu as pltpu
from jax.sharding import PartitionSpec as P

ROUTE_SCALE = 2.5
TM = 256
WIN = 128
ALIGN = 8
CHUNKS = (512,)
CAP = 384
PIECE = 256
MESH = pl.DeviceIdType.MESH


def gate_weights(x_tokens, assign, slot_expert, w_router):
    num_experts, num_slots = w_router.shape[1], slot_expert.shape[0]
    pick = (jnp.arange(num_experts, dtype=jnp.int32)[:, None] == slot_expert[None, :]).astype(w_router.dtype)
    w_slot = jnp.dot(w_router, pick)
    gate_prob = jax.nn.sigmoid(jnp.dot(x_tokens, w_slot, preferred_element_type=jnp.float32))
    hit = assign[:, :, None] == jnp.arange(num_slots, dtype=jnp.int32)
    picked = jnp.sum(jnp.where(hit, gate_prob[:, None, :], 0.0), axis=2)
    gate_total = jnp.sum(picked, axis=1, keepdims=True)
    return ROUTE_SCALE * picked / jnp.maximum(gate_total, 1e-30)


def shared_expert(x_tokens, w1_shared, w3_shared, w2_shared):
    h_gate = jnp.dot(x_tokens, w1_shared, preferred_element_type=jnp.float32)
    h_up = jnp.dot(x_tokens, w3_shared, preferred_element_type=jnp.float32)
    mid_act = (jax.nn.silu(h_gate) * h_up).astype(jnp.bfloat16)
    return jnp.dot(mid_act, w2_shared, preferred_element_type=jnp.float32)


def dispatch(x_all, rank_rows, off, cpad, tail, max_rows):
    blocks, _, tok = rank_rows.shape
    slots = tail.shape[0]
    dim = x_all.shape[1]

    def kernel(off_ref, cpad_ref, tail_ref, rank_ref, x_ref, out_ref, stage, zeros, sem, zsem):
        b = pl.program_id(0)
        buf = lax.rem(b, 2)

        def copy16(i, src_row, dst_row):
            return pltpu.make_async_copy(
                stage.at[i, pl.ds(pl.multiple_of(src_row, ALIGN), ALIGN), :],
                out_ref.at[pl.ds(pl.multiple_of(dst_row, ALIGN), ALIGN), :],
                sem.at[i],
            )

        def drain(step, i):
            total = cpad_ref[step * slots]
            for s in range(1, slots):
                total = total + cpad_ref[step * slots + s]

            def body(_, c):
                copy16(i, 0, 0).wait()
                return c

            lax.fori_loop(0, lax.div(total, ALIGN), body, 0)

        @pl.when(b >= 2)
        def _():
            drain(b - 2, buf)

        rows = lax.broadcasted_iota(jnp.int32, (WIN, tok), 0)
        sel = [(rows == rank_ref[0, s : s + 1, :]).astype(jnp.float32).astype(jnp.bfloat16) for s in range(slots)]
        win = jnp.dot(jnp.concatenate(sel, axis=0), x_ref[...], preferred_element_type=jnp.float32)
        stage[buf] = win.astype(jnp.bfloat16)
        for s in range(slots):
            start = off_ref[b * slots + s]

            def body(c, carry):
                copy16(buf, s * WIN + c * ALIGN, start + c * ALIGN).start()
                return carry

            lax.fori_loop(0, lax.div(cpad_ref[b * slots + s], ALIGN), body, 0)

        @pl.when(b == blocks - 1)
        def _():
            zeros[...] = jnp.zeros_like(zeros)

            def zcopy(row):
                return pltpu.make_async_copy(zeros, out_ref.at[pl.ds(pl.multiple_of(row, ALIGN), ALIGN), :], zsem)

            for wait in (False, True):
                for s in range(slots):
                    first = off_ref[b * slots + s] + cpad_ref[b * slots + s]

                    def body(c, carry):
                        d = zcopy(first + c * ALIGN)
                        d.wait() if wait else d.start()
                        return carry

                    lax.fori_loop(0, lax.div(tail_ref[s] - first, ALIGN), body, 0)
            drain(b - 1, 1 - buf)
            drain(b, buf)

    return pl.pallas_call(
        kernel,
        grid_spec=pltpu.PrefetchScalarGridSpec(
            num_scalar_prefetch=3,
            grid=(blocks,),
            in_specs=[
                pl.BlockSpec((1, rank_rows.shape[1], tok), lambda b, *_: (b, 0, 0)),
                pl.BlockSpec((tok, dim), lambda b, *_: (b, 0)),
            ],
            out_specs=pl.BlockSpec(memory_space=pl.ANY),
            scratch_shapes=[
                pltpu.VMEM((2, slots * WIN, dim), jnp.bfloat16),
                pltpu.VMEM((ALIGN, dim), jnp.bfloat16),
                pltpu.SemaphoreType.DMA((2,)),
                pltpu.SemaphoreType.DMA,
            ],
        ),
        out_shape=jax.ShapeDtypeStruct((max_rows, dim), jnp.bfloat16),
        compiler_params=pltpu.CompilerParams(vmem_limit_bytes=48 * 2**20),
        name="dispatch",
    )(off, cpad, tail, rank_rows, x_all)


def expert_mlp(x_rows, w1, w3, w2, tile_slot, num_tiles, chunk_dst, chunk_count, used, out_rows):
    dim, ff = w1.shape[1:]
    chunks = TM // ALIGN
    parts = out_rows // CAP

    def kernel(slot_ref, tiles_ref, dst_ref, count_ref, used_ref, x_hbm, w1_hbm, w3_hbm, w2_hbm, o_ref, stage, zeros, step, sem, zsem):
        tiles = tiles_ref[0]

        def copy16(k, c, row):
            return pltpu.make_async_copy(
                stage.at[k, pl.ds(pl.multiple_of(c * ALIGN, ALIGN), ALIGN), :],
                o_ref.at[pl.ds(pl.multiple_of(row * ALIGN, ALIGN), ALIGN), :],
                sem.at[k],
            )

        def drain(step, k):
            def body(_, carry):
                copy16(k, 0, 0).wait()
                return carry

            lax.fori_loop(0, count_ref[step], body, 0)

        def zero_fill(wait):
            def part(p, carry):
                def body(c, carry):
                    d = pltpu.make_async_copy(
                        zeros, o_ref.at[pl.ds(pl.multiple_of(p * CAP + c * ALIGN, ALIGN), ALIGN), :], zsem
                    )
                    d.wait() if wait else d.start()
                    return carry

                return lax.fori_loop(used_ref[p], CAP // ALIGN, body, carry)

            lax.fori_loop(0, parts, part, 0)

        zeros[...] = jnp.zeros_like(zeros)
        zero_fill(False)
        step[0] = 0

        def tile(x_ref, w1_ref, w3_ref, w2_ref):
            i = step[0]
            step[0] = i + 1
            buf = lax.rem(i, 2)

            @pl.when(i >= 2)
            def _():
                drain(i - 2, buf)

            def multiply(n):
                x = x_ref[0:n, :]
                gate = jnp.dot(x, w1_ref[0], preferred_element_type=jnp.float32)
                up = jnp.dot(x, w3_ref[0], preferred_element_type=jnp.float32)
                mid = (jax.nn.silu(gate) * up).astype(jnp.bfloat16)
                stage[buf, 0:n, :] = jnp.dot(mid, w2_ref[0], preferred_element_type=jnp.float32).astype(jnp.bfloat16)

            half = TM // 2
            pl.when(count_ref[i] * ALIGN <= half)(lambda: multiply(half))
            pl.when(count_ref[i] * ALIGN > half)(lambda: multiply(TM))

            def body(c, carry):
                copy16(buf, c, dst_ref[i * chunks + c]).start()
                return carry

            lax.fori_loop(0, count_ref[i], body, 0)

        pltpu.emit_pipeline(
            tile,
            grid=(tiles,),
            in_specs=[
                pl.BlockSpec((TM, dim), lambda i: (i, 0)),
                pl.BlockSpec((1, dim, ff), lambda i: (slot_ref[i], 0, 0)),
                pl.BlockSpec((1, dim, ff), lambda i: (slot_ref[i], 0, 0)),
                pl.BlockSpec((1, ff, dim), lambda i: (slot_ref[i], 0, 0)),
            ],
        )(x_hbm, w1_hbm, w3_hbm, w2_hbm)

        @pl.when(tiles >= 2)
        def _():
            drain(tiles - 2, lax.rem(tiles, 2))

        drain(tiles - 1, lax.rem(tiles + 1, 2))
        zero_fill(True)

    return pl.pallas_call(
        kernel,
        in_specs=[pl.BlockSpec(memory_space=pltpu.SMEM)] * 5 + [pl.BlockSpec(memory_space=pl.ANY)] * 4,
        out_specs=pl.BlockSpec(memory_space=pl.ANY),
        scratch_shapes=[
            pltpu.VMEM((2, TM, dim), jnp.bfloat16),
            pltpu.VMEM((ALIGN, dim), jnp.bfloat16),
            pltpu.SMEM((1,), jnp.int32),
            pltpu.SemaphoreType.DMA((2,)),
            pltpu.SemaphoreType.DMA,
        ],
        out_shape=jax.ShapeDtypeStruct((out_rows, dim), jnp.bfloat16),
        compiler_params=pltpu.CompilerParams(vmem_limit_bytes=60 * 2**20),
        name="expert_mlp",
    )(tile_slot, num_tiles.reshape(1), chunk_dst, chunk_count, used, x_rows, w1, w3, w2)


def exchange(o_send, plan, turn, cap):
    dim = o_send.shape[1]
    layers, tok, _ = plan.shape
    pieces = dim // PIECE
    units = layers * pieces
    rows = 4 * cap
    top_k = 6

    def kernel(send_ref, plan_ref, out_ref, recv, zbuf, stage, sel, raw_send, raw_recv, own_sem, z_send, z_recv, out_sem):
        me = lax.axis_index('ep')
        z = me // 4
        q = lax.rem(me, 4)

        def home_of(i):
            low = jnp.where(z == 0, 3 - i, jnp.where(i == 0, 3, jnp.where(i == 1, 0, jnp.where(i == 2, 2, 1))))
            r = 3 - z
            high = jnp.where(r == 0, i, jnp.where(i == 0, 0, jnp.where(i == 1, 3, jnp.where(i == 2, 1, 2))))
            return jnp.where(z < 2, low, high)

        barrier = pltpu.get_barrier_semaphore()
        for d in range(1, 4):
            peer = z * 4 + lax.rem(q + d, 4)
            pl.semaphore_signal(barrier, inc=1, device_id={'ep': peer}, device_id_type=MESH)

        @pl.when(z > 0)
        def _():
            pl.semaphore_signal(barrier, inc=1, device_id={'ep': me - 4}, device_id_type=MESH)

        @pl.when(z < 3)
        def _():
            pl.semaphore_signal(barrier, inc=1, device_id={'ep': me + 4}, device_id_type=MESH)

        pl.semaphore_wait(barrier, 3 + jnp.where(z > 0, 1, 0) + jnp.where(z < 3, 1, 0))

        def block(dst_q, u):
            home, p = home_of(u // pieces), lax.rem(u, pieces)
            row = ((turn * 4 + dst_q) * 4 + home) * CAP
            return send_ref.at[pl.ds(pl.multiple_of(row, 128), cap), pl.ds(pl.multiple_of(p * PIECE, PIECE), PIECE)]

        def raw(d, u):
            dst_q = lax.rem(q + d, 4)
            return pltpu.make_async_remote_copy(
                src_ref=block(dst_q, u),
                dst_ref=recv.at[u, pl.ds(pl.multiple_of(q * cap, cap), cap), :],
                send_sem=raw_send.at[d - 1, u],
                recv_sem=raw_recv.at[d - 1, u],
                device_id={'ep': z * 4 + dst_q},
                device_id_type=MESH,
            )

        def own(u):
            return pltpu.make_async_copy(
                block(q, u), recv.at[u, pl.ds(pl.multiple_of(q * cap, cap), cap), :], own_sem.at[u]
            )

        def start_raw(u, carry):
            for d in range(1, 4):
                raw(d, u).start()
            own(u).start()
            return carry

        lax.fori_loop(0, units, start_raw, 0)

        def up(slot, u):
            return pltpu.make_async_remote_copy(
                src_ref=stage.at[lax.rem(u, 4)],
                dst_ref=zbuf.at[slot, lax.rem(u, pieces)],
                send_sem=z_send.at[lax.rem(u, 4)],
                recv_sem=z_recv.at[slot, lax.rem(u, pieces)],
                device_id={'ep': me + 4},
                device_id_type=MESH,
            )

        def down(slot, u):
            return pltpu.make_async_remote_copy(
                src_ref=stage.at[lax.rem(u, 4)],
                dst_ref=zbuf.at[slot, lax.rem(u, pieces)],
                send_sem=z_send.at[lax.rem(u, 4)],
                recv_sem=z_recv.at[slot, lax.rem(u, pieces)],
                device_id={'ep': me - 4},
                device_id_type=MESH,
            )

        def finish(u):
            p = lax.rem(u, pieces)
            return pltpu.make_async_copy(
                stage.at[lax.rem(u, 4)], out_ref.at[:, pl.ds(pl.multiple_of(p * PIECE, PIECE), PIECE)], out_sem.at[p]
            )

        def unit(u, carry):
            home, p = home_of(u // pieces), lax.rem(u, pieces)
            k = lax.rem(u, 4)

            @pl.when(p == 0)
            def _():
                lanes = lax.broadcasted_iota(jnp.int32, (tok, cap), 1).astype(jnp.float32)
                mine = plan_ref[home]
                for src in range(4):
                    a = jnp.zeros((tok, cap), jnp.float32)
                    for c in range(top_k):
                        a = jnp.where(lanes == mine[:, c : c + 1] - float(src * cap), mine[:, 8 + c : 9 + c], a)
                    hi = a.astype(jnp.bfloat16)
                    rest = a - hi.astype(jnp.float32)
                    mid = rest.astype(jnp.bfloat16)
                    sel[0, :, src * cap : (src + 1) * cap] = hi
                    sel[1, :, src * cap : (src + 1) * cap] = mid
                    sel[2, :, src * cap : (src + 1) * cap] = (rest - mid.astype(jnp.float32)).astype(jnp.bfloat16)

            for d in range(1, 4):
                raw(d, u).wait()
            own(u).wait()

            @pl.when((u >= 4) & (u < units - pieces + 4))
            def _():
                up(0, u - 4).wait_send()

            @pl.when(u >= units - pieces + 4)
            def _():
                finish(u - 4).wait()

            stage[k] = jnp.dot(sel[0], recv[u], preferred_element_type=jnp.float32)

            def term(j, c):
                stage[k] += jnp.dot(sel[j], recv[u], preferred_element_type=jnp.float32)
                return c

            lax.fori_loop(1, 3, term, 0)

            @pl.when(((home < z) & (z < 3)) | ((home >= z) & (z > 0)))
            def _():
                up(home, u).wait_recv()
                stage[k] += zbuf[home, p]

            @pl.when((home == z) & (z < 3))
            def _():
                up(4, u).wait_recv()
                stage[k] += zbuf[4, p]

            @pl.when(home > z)
            def _():
                up(home, u).start()

            @pl.when(home < z)
            def _():
                down(jnp.where(home == z - 1, 4, home), u).start()

            @pl.when(home == z)
            def _():
                finish(u).start()

            return carry

        lax.fori_loop(0, units, unit, 0)
        for u in range(units - 4, units):
            finish(u).wait()

    return pl.pallas_call(
        kernel,
        out_shape=jax.ShapeDtypeStruct((tok, dim), jnp.float32),
        in_specs=[pl.BlockSpec(memory_space=pl.ANY), pl.BlockSpec(memory_space=pltpu.VMEM)],
        out_specs=pl.BlockSpec(memory_space=pl.ANY),
        scratch_shapes=[
            pltpu.VMEM((units, rows, PIECE), jnp.bfloat16),
            pltpu.VMEM((5, pieces, tok, PIECE), jnp.float32),
            pltpu.VMEM((4, tok, PIECE), jnp.float32),
            pltpu.VMEM((3, tok, rows), jnp.bfloat16),
            pltpu.SemaphoreType.DMA((3, units)),
            pltpu.SemaphoreType.DMA((3, units)),
            pltpu.SemaphoreType.DMA((units,)),
            pltpu.SemaphoreType.DMA((4,)),
            pltpu.SemaphoreType.DMA((5, pieces)),
            pltpu.SemaphoreType.DMA((pieces,)),
        ],
        compiler_params=pltpu.CompilerParams(
            collective_id=1 + turn, has_side_effects=True, vmem_limit_bytes=66_000_000
        ),
        name="exchange",
    )(o_send, plan)


def running_count(assign_all, num_slots):
    tok = assign_all.shape[1]
    member = jnp.any(assign_all[..., None] == jnp.arange(num_slots, dtype=jnp.int32), axis=2)
    upto = (jnp.arange(tok)[:, None] >= jnp.arange(tok)[None, :]).astype(jnp.bfloat16)
    order = jnp.einsum('pq,bqs->bps', upto, member.astype(jnp.bfloat16), preferred_element_type=jnp.float32)
    return member, order.astype(jnp.int32)


def solution(mesh):
    group_size = mesh.shape['ep']

    def device_step(x_tokens, slot_expert, w1_slots, w3_slots, w2_slots, assign, w_router, w1_shared, w3_shared, w2_shared):
        tok, dim = x_tokens.shape
        top_k = assign.shape[1]
        slots = w1_slots.shape[0]
        num_slots = slots * group_size
        me = lax.axis_index('ep')
        my_z, my_q = me // 4, me % 4
        max_tiles = slots * (group_size * WIN // TM)
        chunks = TM // ALIGN
        weight = gate_weights(x_tokens, assign, slot_expert, w_router)
        ends = [sum(CHUNKS[: c + 1]) for c in range(len(CHUNKS))]
        x_chunks = [lax.all_gather(x_tokens[e - t : e], 'ep', tiled=True) for t, e in zip(CHUNKS, ends)]
        meta = lax.all_gather(jnp.concatenate([assign.astype(jnp.float32), weight], axis=1), ('dp', 'ep'))
        meta = meta.reshape(-1, group_size, tok, 2 * top_k)
        everyone = meta[..., :top_k].astype(jnp.int32)
        my_dp = lax.axis_index('dp')
        assign_all = lax.dynamic_index_in_dim(everyone, my_dp, 0, keepdims=False)
        w_all = lax.dynamic_index_in_dim(meta, my_dp, 0, keepdims=False)[..., top_k:]

        def padded(count):
            return (count + ALIGN - 1) // ALIGN * ALIGN

        member_e = jnp.any(everyone[..., None] == jnp.arange(num_slots, dtype=jnp.int32), axis=3)
        need = sum(
            jnp.sum(padded(jnp.sum(member_e[:, :, e - t : e].astype(jnp.int32), axis=2)).reshape(-1, group_size, slots), axis=2)
            for t, e in zip(CHUNKS, ends)
        )
        crowded = jnp.max(need) > CAP

        member, order = running_count(assign_all, num_slots)
        totals = jnp.stack([order[:, e - 1, :] for e in ends])
        starts = jnp.concatenate([jnp.zeros_like(totals[:1]), totals[:-1]])
        cpad = padded(totals - starts)
        by_dev = jnp.transpose(cpad.reshape(len(CHUNKS), group_size, group_size, slots), (1, 2, 3, 0))
        split = CAP // WIN
        in_turn = jnp.where(crowded & (jnp.arange(slots) >= split), 1, 0)
        flat = by_dev.reshape(group_size, group_size, -1)
        before = (jnp.cumsum(flat, axis=2) - flat).reshape(by_dev.shape)
        place = before - jnp.where(in_turn[:, None] == 1, before[:, :, split : split + 1, :1], 0)
        place = jnp.transpose(place, (3, 0, 1, 2))
        turn_of = jnp.broadcast_to(in_turn, (group_size, slots)).reshape(num_slots)

        my_pad = lax.dynamic_slice_in_dim(cpad, me * slots, slots, axis=2)
        my_start = lax.dynamic_slice_in_dim(starts, me * slots, slots, axis=2)
        my_order = lax.dynamic_slice_in_dim(order, me * slots, slots, axis=2)
        my_member = lax.dynamic_slice_in_dim(member, me * slots, slots, axis=2)
        my_place = lax.dynamic_slice_in_dim(place, me, 1, axis=2)[:, :, 0]
        home = jnp.arange(group_size, dtype=jnp.int32)
        base = (in_turn[None, :] * 16 + ((home % 4) * 4 + home // 4)[:, None]) * CAP
        tile_ids = jnp.arange(max_tiles, dtype=jnp.int32)
        row0 = jnp.arange(max_tiles * chunks, dtype=jnp.int32) * ALIGN

        def chunk_plan(c):
            t, e, mine = CHUNKS[c], ends[c], my_pad[c]
            tiles = (jnp.sum(mine, axis=0) + TM - 1) // TM
            tile_end = jnp.cumsum(tiles)
            off = ((tile_end - tiles) * TM)[None, :] + jnp.cumsum(mine, axis=0) - mine
            num_tiles = jnp.maximum(tile_end[-1], 1)
            tile_slot = jnp.sum((jnp.minimum(tile_ids, num_tiles - 1)[:, None] >= tile_end[None, :-1]).astype(jnp.int32), axis=1)
            tail = jnp.concatenate([tile_end[:-1], num_tiles[None]]) * TM
            rank = jnp.where(my_member[:, e - t : e], my_order[:, e - t : e] - my_start[c][:, None, :] - 1, -1)
            rank_rows = jnp.pad(jnp.transpose(rank, (0, 2, 1)), ((0, 0), (0, 8 - slots), (0, 0)), constant_values=-1)
            lo, hi = off.reshape(-1), (off + mine).reshape(-1)
            inside = (row0[:, None] >= lo[None, :]) & (row0[:, None] < hi[None, :])
            shift = (base + my_place[c] - off).reshape(-1)
            dst = jnp.sum(jnp.where(inside, shift[None, :] + row0[:, None], 0), axis=1) // ALIGN
            count = jnp.sum(inside.reshape(max_tiles, chunks, -1).astype(jnp.int32), axis=(1, 2))
            return (rank_rows, off.reshape(-1), mine.reshape(-1), tail), (tile_slot, num_tiles, dst, count)

        mine = jnp.sum(my_pad, axis=0)
        filled = jnp.stack(
            [jnp.sum(jnp.where(in_turn == 0, mine, 0), axis=1), jnp.where(crowded, jnp.sum(jnp.where(in_turn == 1, mine, 0), axis=1), CAP)]
        )
        used = jnp.transpose(filled.reshape(2, 4, 4), (0, 2, 1)).reshape(-1) // ALIGN

        sum_order = lax.dynamic_slice_in_dim(order.reshape(4, 4, tok, num_slots), my_q, 1, axis=1)[:, 0]
        sum_place = lax.dynamic_slice_in_dim((place.reshape(starts.shape) - starts).reshape(-1, 4, 4, num_slots), my_q, 1, axis=2)[:, :, 0]
        sum_assign = lax.dynamic_slice_in_dim(assign_all.reshape(4, 4, tok, top_k), my_q, 1, axis=1)[:, 0]
        sum_weight = lax.dynamic_slice_in_dim(w_all.reshape(4, 4, tok, top_k), my_q, 1, axis=1)[:, 0]
        slot_ids = jnp.arange(num_slots, dtype=jnp.int32)
        arrives = jnp.where(slot_ids // (4 * slots) == my_z, (slot_ids // slots) % 4 * CAP + sum_place, -(2**20))
        arrives = jnp.concatenate(
            [jnp.broadcast_to(arrives[c][:, None, :], (4, t, num_slots)) for c, t in enumerate(CHUNKS)], axis=1
        ) + sum_order
        hit = sum_assign[..., None] == slot_ids

        def plan_of(turn):
            col = jnp.sum(jnp.where(hit & (turn_of == turn), arrives[:, :, None, :], 0), axis=3) - 1
            pad = ((0, 0), (0, 0), (0, 8 - top_k))
            return jnp.concatenate(
                [jnp.pad(col.astype(jnp.float32), pad, constant_values=-1.0), jnp.pad(sum_weight, pad)], axis=2
            )

        plans = [chunk_plan(c) for c in range(len(CHUNKS))]
        shared_out = shared_expert(x_tokens, w1_shared, w3_shared, w2_shared)
        x_chunks[0], shared_out = lax.optimization_barrier((x_chunks[0], shared_out))
        o_send = 32 * CAP
        for x_part, (rows_plan, tiles_plan) in zip(x_chunks, plans):
            x_rows = dispatch(x_part, *rows_plan, max_tiles * TM)
            o_send = expert_mlp(x_rows, w1_slots, w3_slots, w2_slots, *tiles_plan, used, o_send)
        routed = exchange(o_send, plan_of(0), 0, CAP)
        routed = lax.cond(
            crowded, lambda r, o, p: r + exchange(o, p, 1, CAP), lambda r, o, p: r, routed, o_send, plan_of(1)
        )
        return (shared_out + routed).astype(jnp.bfloat16)

    token_spec = P(('dp', 'ep'), None)
    slot_spec = P('ep', None, None)
    return jax.shard_map(device_step, mesh=mesh, in_specs=(token_spec, P(), slot_spec, slot_spec, slot_spec, token_spec, P(), P(), P(), P()), out_specs=token_spec, check_vma=False)
```

```python
import jax
import jax.numpy as jnp
from jax import lax
from jax.experimental import pallas as pl
from jax.experimental.pallas import tpu as pltpu
from jax.sharding import PartitionSpec as P

ROUTE_SCALE = 2.5
TM = 256
WIN = 128
ALIGN = 8
CAP = 384
PIECE = 256
MESH = pl.DeviceIdType.MESH


def gate_weights(x_tokens, assign, slot_expert, w_router):
    num_experts, num_slots = w_router.shape[1], slot_expert.shape[0]
    pick = (jnp.arange(num_experts, dtype=jnp.int32)[:, None] == slot_expert[None, :]).astype(w_router.dtype)
    w_slot = jnp.dot(w_router, pick)
    gate_prob = jax.nn.sigmoid(jnp.dot(x_tokens, w_slot, preferred_element_type=jnp.float32))
    hit = assign[:, :, None] == jnp.arange(num_slots, dtype=jnp.int32)
    picked = jnp.sum(jnp.where(hit, gate_prob[:, None, :], 0.0), axis=2)
    gate_total = jnp.sum(picked, axis=1, keepdims=True)
    return ROUTE_SCALE * picked / jnp.maximum(gate_total, 1e-30)


def shared_expert(x_tokens, w1_shared, w3_shared, w2_shared):
    h_gate = jnp.dot(x_tokens, w1_shared, preferred_element_type=jnp.float32)
    h_up = jnp.dot(x_tokens, w3_shared, preferred_element_type=jnp.float32)
    mid_act = (jax.nn.silu(h_gate) * h_up).astype(jnp.bfloat16)
    return jnp.dot(mid_act, w2_shared, preferred_element_type=jnp.float32)


def dispatch(x_all, rank_rows, off, cpad, tail, max_rows):
    blocks, _, tok = rank_rows.shape
    slots = tail.shape[0]
    dim = x_all.shape[1]

    def kernel(off_ref, cpad_ref, tail_ref, rank_ref, x_ref, out_ref, stage, zeros, sem, zsem):
        b = pl.program_id(0)
        buf = lax.rem(b, 2)

        def copy16(i, src_row, dst_row):
            return pltpu.make_async_copy(
                stage.at[i, pl.ds(pl.multiple_of(src_row, ALIGN), ALIGN), :],
                out_ref.at[pl.ds(pl.multiple_of(dst_row, ALIGN), ALIGN), :],
                sem.at[i],
            )

        def drain(step, i):
            total = cpad_ref[step * slots]
            for s in range(1, slots):
                total = total + cpad_ref[step * slots + s]

            def body(_, c):
                copy16(i, 0, 0).wait()
                return c

            lax.fori_loop(0, lax.div(total, ALIGN), body, 0)

        @pl.when(b >= 2)
        def _():
            drain(b - 2, buf)

        rows = lax.broadcasted_iota(jnp.int32, (WIN, tok), 0)
        sel = [(rows == rank_ref[0, s : s + 1, :]).astype(jnp.float32).astype(jnp.bfloat16) for s in range(slots)]
        win = jnp.dot(jnp.concatenate(sel, axis=0), x_ref[...], preferred_element_type=jnp.float32)
        stage[buf] = win.astype(jnp.bfloat16)
        for s in range(slots):
            start = off_ref[b * slots + s]

            def body(c, carry):
                copy16(buf, s * WIN + c * ALIGN, start + c * ALIGN).start()
                return carry

            lax.fori_loop(0, lax.div(cpad_ref[b * slots + s], ALIGN), body, 0)

        @pl.when(b == blocks - 1)
        def _():
            zeros[...] = jnp.zeros_like(zeros)

            def zcopy(row):
                return pltpu.make_async_copy(zeros, out_ref.at[pl.ds(pl.multiple_of(row, ALIGN), ALIGN), :], zsem)

            for wait in (False, True):
                for s in range(slots):
                    first = off_ref[b * slots + s] + cpad_ref[b * slots + s]

                    def body(c, carry):
                        d = zcopy(first + c * ALIGN)
                        d.wait() if wait else d.start()
                        return carry

                    lax.fori_loop(0, lax.div(tail_ref[s] - first, ALIGN), body, 0)
            drain(b - 1, 1 - buf)
            drain(b, buf)

    return pl.pallas_call(
        kernel,
        grid_spec=pltpu.PrefetchScalarGridSpec(
            num_scalar_prefetch=3,
            grid=(blocks,),
            in_specs=[
                pl.BlockSpec((1, rank_rows.shape[1], tok), lambda b, *_: (b, 0, 0)),
                pl.BlockSpec((tok, dim), lambda b, *_: (b, 0)),
            ],
            out_specs=pl.BlockSpec(memory_space=pl.ANY),
            scratch_shapes=[
                pltpu.VMEM((2, slots * WIN, dim), jnp.bfloat16),
                pltpu.VMEM((ALIGN, dim), jnp.bfloat16),
                pltpu.SemaphoreType.DMA((2,)),
                pltpu.SemaphoreType.DMA,
            ],
        ),
        out_shape=jax.ShapeDtypeStruct((max_rows, dim), jnp.bfloat16),
        compiler_params=pltpu.CompilerParams(vmem_limit_bytes=48 * 2**20),
        name="dispatch",
    )(off, cpad, tail, rank_rows, x_all)


def expert_mlp(x_rows, w1, w3, w2, tile_slot, num_tiles, chunk_dst, chunk_count, used, out_rows):
    dim, ff = w1.shape[1:]
    chunks = TM // ALIGN
    parts = out_rows // CAP

    def kernel(slot_ref, tiles_ref, dst_ref, count_ref, used_ref, x_hbm, w1_hbm, w3_hbm, w2_hbm, o_ref, stage, zeros, step, sem, zsem):
        tiles = tiles_ref[0]

        def copy16(k, c, row):
            return pltpu.make_async_copy(
                stage.at[k, pl.ds(pl.multiple_of(c * ALIGN, ALIGN), ALIGN), :],
                o_ref.at[pl.ds(pl.multiple_of(row * ALIGN, ALIGN), ALIGN), :],
                sem.at[k],
            )

        def drain(step, k):
            def body(_, carry):
                copy16(k, 0, 0).wait()
                return carry

            lax.fori_loop(0, count_ref[step], body, 0)

        def zero_fill(wait):
            def part(p, carry):
                def body(c, carry):
                    d = pltpu.make_async_copy(
                        zeros, o_ref.at[pl.ds(pl.multiple_of(p * CAP + c * ALIGN, ALIGN), ALIGN), :], zsem
                    )
                    d.wait() if wait else d.start()
                    return carry

                return lax.fori_loop(used_ref[p], CAP // ALIGN, body, carry)

            lax.fori_loop(0, parts, part, 0)

        zeros[...] = jnp.zeros_like(zeros)
        zero_fill(False)
        step[0] = 0

        def tile(x_ref, w1_ref, w3_ref, w2_ref):
            i = step[0]
            step[0] = i + 1
            buf = lax.rem(i, 2)

            @pl.when(i >= 2)
            def _():
                drain(i - 2, buf)

            def multiply(n):
                x = x_ref[0:n, :]
                gate = jnp.dot(x, w1_ref[0], preferred_element_type=jnp.float32)
                up = jnp.dot(x, w3_ref[0], preferred_element_type=jnp.float32)
                mid = (jax.nn.silu(gate) * up).astype(jnp.bfloat16)
                stage[buf, 0:n, :] = jnp.dot(mid, w2_ref[0], preferred_element_type=jnp.float32).astype(jnp.bfloat16)

            half = TM // 2
            pl.when(count_ref[i] * ALIGN <= half)(lambda: multiply(half))
            pl.when(count_ref[i] * ALIGN > half)(lambda: multiply(TM))

            def body(c, carry):
                copy16(buf, c, dst_ref[i * chunks + c]).start()
                return carry

            lax.fori_loop(0, count_ref[i], body, 0)

        pltpu.emit_pipeline(
            tile,
            grid=(tiles,),
            in_specs=[
                pl.BlockSpec((TM, dim), lambda i: (i, 0)),
                pl.BlockSpec((1, dim, ff), lambda i: (slot_ref[i], 0, 0)),
                pl.BlockSpec((1, dim, ff), lambda i: (slot_ref[i], 0, 0)),
                pl.BlockSpec((1, ff, dim), lambda i: (slot_ref[i], 0, 0)),
            ],
        )(x_hbm, w1_hbm, w3_hbm, w2_hbm)

        @pl.when(tiles >= 2)
        def _():
            drain(tiles - 2, lax.rem(tiles, 2))

        drain(tiles - 1, lax.rem(tiles + 1, 2))
        zero_fill(True)

    return pl.pallas_call(
        kernel,
        in_specs=[pl.BlockSpec(memory_space=pltpu.SMEM)] * 5 + [pl.BlockSpec(memory_space=pl.ANY)] * 4,
        out_specs=pl.BlockSpec(memory_space=pl.ANY),
        scratch_shapes=[
            pltpu.VMEM((2, TM, dim), jnp.bfloat16),
            pltpu.VMEM((ALIGN, dim), jnp.bfloat16),
            pltpu.SMEM((1,), jnp.int32),
            pltpu.SemaphoreType.DMA((2,)),
            pltpu.SemaphoreType.DMA,
        ],
        out_shape=jax.ShapeDtypeStruct((out_rows, dim), jnp.bfloat16),
        compiler_params=pltpu.CompilerParams(vmem_limit_bytes=60 * 2**20),
        name="expert_mlp",
    )(tile_slot, num_tiles.reshape(1), chunk_dst, chunk_count, used, x_rows, w1, w3, w2)


def exchange(o_send, plan, turn, cap):
    dim = o_send.shape[1]
    layers, tok, _ = plan.shape
    pieces = dim // PIECE
    units = layers * pieces
    rows = 4 * cap
    top_k = 6

    def kernel(send_ref, plan_ref, out_ref, recv, zbuf, stage, sel, raw_send, raw_recv, own_sem, z_send, z_recv, out_sem):
        me = lax.axis_index('ep')
        z = me // 4
        q = lax.rem(me, 4)

        def home_of(i):
            low = jnp.where(z == 0, 3 - i, jnp.where(i == 0, 3, jnp.where(i == 1, 0, jnp.where(i == 2, 2, 1))))
            r = 3 - z
            high = jnp.where(r == 0, i, jnp.where(i == 0, 0, jnp.where(i == 1, 3, jnp.where(i == 2, 1, 2))))
            return jnp.where(z < 2, low, high)

        barrier = pltpu.get_barrier_semaphore()
        for d in range(1, 4):
            peer = z * 4 + lax.rem(q + d, 4)
            pl.semaphore_signal(barrier, inc=1, device_id={'ep': peer}, device_id_type=MESH)

        @pl.when(z > 0)
        def _():
            pl.semaphore_signal(barrier, inc=1, device_id={'ep': me - 4}, device_id_type=MESH)

        @pl.when(z < 3)
        def _():
            pl.semaphore_signal(barrier, inc=1, device_id={'ep': me + 4}, device_id_type=MESH)

        pl.semaphore_wait(barrier, 3 + jnp.where(z > 0, 1, 0) + jnp.where(z < 3, 1, 0))

        def block(dst_q, u):
            home, p = home_of(u // pieces), lax.rem(u, pieces)
            row = ((turn * 4 + dst_q) * 4 + home) * CAP
            return send_ref.at[pl.ds(pl.multiple_of(row, 128), cap), pl.ds(pl.multiple_of(p * PIECE, PIECE), PIECE)]

        def raw(d, u):
            dst_q = lax.rem(q + d, 4)
            return pltpu.make_async_remote_copy(
                src_ref=block(dst_q, u),
                dst_ref=recv.at[u, pl.ds(pl.multiple_of(q * cap, cap), cap), :],
                send_sem=raw_send.at[d - 1, u],
                recv_sem=raw_recv.at[d - 1, u],
                device_id={'ep': z * 4 + dst_q},
                device_id_type=MESH,
            )

        def own(u):
            return pltpu.make_async_copy(
                block(q, u), recv.at[u, pl.ds(pl.multiple_of(q * cap, cap), cap), :], own_sem.at[u]
            )

        def start_raw(u, carry):
            for d in range(1, 4):
                raw(d, u).start()
            own(u).start()
            return carry

        lax.fori_loop(0, units, start_raw, 0)

        def up(slot, u):
            return pltpu.make_async_remote_copy(
                src_ref=stage.at[lax.rem(u, 4)],
                dst_ref=zbuf.at[slot, lax.rem(u, pieces)],
                send_sem=z_send.at[lax.rem(u, 4)],
                recv_sem=z_recv.at[slot, lax.rem(u, pieces)],
                device_id={'ep': me + 4},
                device_id_type=MESH,
            )

        def down(slot, u):
            return pltpu.make_async_remote_copy(
                src_ref=stage.at[lax.rem(u, 4)],
                dst_ref=zbuf.at[slot, lax.rem(u, pieces)],
                send_sem=z_send.at[lax.rem(u, 4)],
                recv_sem=z_recv.at[slot, lax.rem(u, pieces)],
                device_id={'ep': me - 4},
                device_id_type=MESH,
            )

        def finish(u):
            p = lax.rem(u, pieces)
            return pltpu.make_async_copy(
                stage.at[lax.rem(u, 4)], out_ref.at[:, pl.ds(pl.multiple_of(p * PIECE, PIECE), PIECE)], out_sem.at[p]
            )

        def unit(u, carry):
            home, p = home_of(u // pieces), lax.rem(u, pieces)
            k = lax.rem(u, 4)

            @pl.when(p == 0)
            def _():
                lanes = lax.broadcasted_iota(jnp.int32, (tok, cap), 1).astype(jnp.float32)
                mine = plan_ref[home]
                for src in range(4):
                    a = jnp.zeros((tok, cap), jnp.float32)
                    for c in range(top_k):
                        a = jnp.where(lanes == mine[:, c : c + 1] - float(src * cap), mine[:, 8 + c : 9 + c], a)
                    hi = a.astype(jnp.bfloat16)
                    rest = a - hi.astype(jnp.float32)
                    mid = rest.astype(jnp.bfloat16)
                    sel[0, :, src * cap : (src + 1) * cap] = hi
                    sel[1, :, src * cap : (src + 1) * cap] = mid
                    sel[2, :, src * cap : (src + 1) * cap] = (rest - mid.astype(jnp.float32)).astype(jnp.bfloat16)

            for d in range(1, 4):
                raw(d, u).wait()
            own(u).wait()

            @pl.when((u >= 4) & (u < units - pieces + 4))
            def _():
                up(0, u - 4).wait_send()

            @pl.when(u >= units - pieces + 4)
            def _():
                finish(u - 4).wait()

            stage[k] = jnp.dot(sel[0], recv[u], preferred_element_type=jnp.float32)

            def term(j, c):
                stage[k] += jnp.dot(sel[j], recv[u], preferred_element_type=jnp.float32)
                return c

            lax.fori_loop(1, 3, term, 0)

            @pl.when(((home < z) & (z < 3)) | ((home >= z) & (z > 0)))
            def _():
                up(home, u).wait_recv()
                stage[k] += zbuf[home, p]

            @pl.when((home == z) & (z < 3))
            def _():
                up(4, u).wait_recv()
                stage[k] += zbuf[4, p]

            @pl.when(home > z)
            def _():
                up(home, u).start()

            @pl.when(home < z)
            def _():
                down(jnp.where(home == z - 1, 4, home), u).start()

            @pl.when(home == z)
            def _():
                finish(u).start()

            return carry

        lax.fori_loop(0, units, unit, 0)
        for u in range(units - 4, units):
            finish(u).wait()

    return pl.pallas_call(
        kernel,
        out_shape=jax.ShapeDtypeStruct((tok, dim), jnp.float32),
        in_specs=[pl.BlockSpec(memory_space=pl.ANY), pl.BlockSpec(memory_space=pltpu.VMEM)],
        out_specs=pl.BlockSpec(memory_space=pl.ANY),
        scratch_shapes=[
            pltpu.VMEM((units, rows, PIECE), jnp.bfloat16),
            pltpu.VMEM((5, pieces, tok, PIECE), jnp.float32),
            pltpu.VMEM((4, tok, PIECE), jnp.float32),
            pltpu.VMEM((3, tok, rows), jnp.bfloat16),
            pltpu.SemaphoreType.DMA((3, units)),
            pltpu.SemaphoreType.DMA((3, units)),
            pltpu.SemaphoreType.DMA((units,)),
            pltpu.SemaphoreType.DMA((4,)),
            pltpu.SemaphoreType.DMA((5, pieces)),
            pltpu.SemaphoreType.DMA((pieces,)),
        ],
        compiler_params=pltpu.CompilerParams(
            collective_id=1 + turn, has_side_effects=True, vmem_limit_bytes=66_000_000
        ),
        name="exchange",
    )(o_send, plan)


def slot_shares(same, counts, slots):
    n = counts.shape[1]

    def kernel(same_ref, count_ref, share_ref):
        same = same_ref[...]
        count = count_ref[...]
        eye = lax.broadcasted_iota(jnp.int32, (n, n), 0) == lax.broadcasted_iota(jnp.int32, (n, n), 1)
        dev = lax.broadcasted_iota(jnp.int32, (n, n), 0) // slots == lax.broadcasted_iota(jnp.int32, (n, n), 1) // slots

        def column(row):
            return jnp.sum(jnp.where(eye, row, 0.0), axis=1, keepdims=True)

        def total(mask, row):
            return jnp.sum(jnp.where(mask, column(row), 0.0), axis=0, keepdims=True)

        one = same > 0.5
        share = 1.0 / total(one, jnp.ones_like(count))
        mean = jnp.sum(share * count) / float(n // slots)

        def step(_, share):
            load = total(dev, share * count)
            share = share * jnp.exp(jnp.clip(1.5 * (1.0 - load / jnp.maximum(mean, 1.0)), -2.0, 2.0))
            share = jnp.maximum(share, 1e-3)
            return share / total(one, share)

        share_ref[...] = lax.fori_loop(0, 24, step, share)

    return pl.pallas_call(
        kernel,
        out_shape=jax.ShapeDtypeStruct((1, n), jnp.float32),
        name="slot_shares",
    )(same, counts)


def place_choices(expert_all, slot_expert, slots):
    tok = expert_all.shape[1]
    num_slots = slot_expert.shape[0]
    wants = jnp.any(expert_all[..., None] == slot_expert, axis=2)
    upto = (jnp.arange(tok)[:, None] >= jnp.arange(tok)[None, :]).astype(jnp.bfloat16)
    order = jnp.einsum('pq,bqs->bps', upto, wants.astype(jnp.bfloat16), preferred_element_type=jnp.float32)
    count = order[:, -1, :]
    same = slot_expert[:, None] == slot_expert[None, :]
    ids = jnp.arange(num_slots)
    earlier = same & (ids[None, :] < ids[:, None])
    copy_no = jnp.sum(earlier, axis=1)
    nxt = same & (copy_no[None, :] == copy_no[:, None] + 1)
    has_next = jnp.any(nxt, axis=1)
    group = jnp.sum(count, axis=0, keepdims=True)
    share = slot_shares(same.astype(jnp.float32), group, slots)

    def bounds(begin):
        lo = jnp.floor(count * begin)
        after = jnp.sum(jnp.where(nxt, begin[:, None, :], 0.0), axis=2)
        return lo, jnp.where(has_next, jnp.floor(count * after), count)

    lo, hi = bounds(jnp.sum(jnp.where(earlier, share, 0.0), axis=1)[None, :])
    even_lo, even_hi = bounds((copy_no / jnp.sum(same, axis=1)).astype(jnp.float32)[None, :])
    over = jnp.max(hi - lo) > 115.0
    lo, hi = jnp.where(over, even_lo, lo), jnp.where(over, even_hi, hi)
    member = wants & (order > lo[:, None, :]) & (order <= hi[:, None, :])
    return member, (order - lo[:, None, :]).astype(jnp.int32), (hi - lo).astype(jnp.int32)


def solution(mesh):
    group_size = mesh.shape['ep']

    def device_step(x_tokens, slot_expert, w1_slots, w3_slots, w2_slots, assign, w_router, w1_shared, w3_shared, w2_shared):
        tok, dim = x_tokens.shape
        top_k = assign.shape[1]
        slots = w1_slots.shape[0]
        num_slots = slots * group_size
        me = lax.axis_index('ep')
        my_z, my_q = me // 4, me % 4
        max_tiles = slots * (group_size * WIN // TM)
        chunks = TM // ALIGN
        weight = gate_weights(x_tokens, assign, slot_expert, w_router)
        x_all = lax.all_gather(x_tokens, 'ep', tiled=True)
        slot_hit = assign[:, :, None] == jnp.arange(num_slots, dtype=jnp.int32)
        expert = jnp.sum(jnp.where(slot_hit, slot_expert + 1, 0), axis=2) - 1
        meta = lax.all_gather(jnp.concatenate([expert.astype(jnp.float32), weight], axis=1), 'ep')
        expert_all = meta[..., :top_k].astype(jnp.int32)
        w_all = meta[..., top_k:]

        def padded(count):
            return (count + ALIGN - 1) // ALIGN * ALIGN

        member, order, count = place_choices(expert_all, slot_expert, slots)
        cpad = padded(count)
        by_dev = cpad.reshape(group_size, group_size, slots)
        crowded = jnp.max(jnp.sum(by_dev, axis=2)) > CAP
        crowded = lax.pmax(crowded.astype(jnp.int32), ('dp', 'ep')) > 0
        split = CAP // WIN
        in_turn = jnp.where(crowded & (jnp.arange(slots) >= split), 1, 0)
        before = jnp.cumsum(by_dev, axis=2) - by_dev
        place = before - jnp.where(in_turn == 1, before[:, :, split : split + 1], 0)
        turn_of = jnp.broadcast_to(in_turn, (group_size, slots)).reshape(num_slots)

        mine = lax.dynamic_slice_in_dim(cpad, me * slots, slots, axis=1)
        my_order = lax.dynamic_slice_in_dim(order, me * slots, slots, axis=2)
        my_member = lax.dynamic_slice_in_dim(member, me * slots, slots, axis=2)
        my_place = lax.dynamic_slice_in_dim(place, me, 1, axis=1)[:, 0]
        home = jnp.arange(group_size, dtype=jnp.int32)
        base = (in_turn[None, :] * 16 + ((home % 4) * 4 + home // 4)[:, None]) * CAP
        tile_ids = jnp.arange(max_tiles, dtype=jnp.int32)
        row0 = jnp.arange(max_tiles * chunks, dtype=jnp.int32) * ALIGN

        tiles = (jnp.sum(mine, axis=0) + TM - 1) // TM
        tile_end = jnp.cumsum(tiles)
        off = ((tile_end - tiles) * TM)[None, :] + jnp.cumsum(mine, axis=0) - mine
        num_tiles = jnp.maximum(tile_end[-1], 1)
        tile_slot = jnp.sum((jnp.minimum(tile_ids, num_tiles - 1)[:, None] >= tile_end[None, :-1]).astype(jnp.int32), axis=1)
        tail = jnp.concatenate([tile_end[:-1], num_tiles[None]]) * TM
        rank = jnp.where(my_member, my_order - 1, -1)
        rank_rows = jnp.pad(jnp.transpose(rank, (0, 2, 1)), ((0, 0), (0, 8 - slots), (0, 0)), constant_values=-1)
        lo, hi = off.reshape(-1), (off + mine).reshape(-1)
        inside = (row0[:, None] >= lo[None, :]) & (row0[:, None] < hi[None, :])
        shift = (base + my_place - off).reshape(-1)
        chunk_dst = jnp.sum(jnp.where(inside, shift[None, :] + row0[:, None], 0), axis=1) // ALIGN
        chunk_count = jnp.sum(inside.reshape(max_tiles, chunks, -1).astype(jnp.int32), axis=(1, 2))
        filled = jnp.stack(
            [jnp.sum(jnp.where(in_turn == 0, mine, 0), axis=1), jnp.where(crowded, jnp.sum(jnp.where(in_turn == 1, mine, 0), axis=1), CAP)]
        )
        used = jnp.transpose(filled.reshape(2, 4, 4), (0, 2, 1)).reshape(-1) // ALIGN

        def of_my_homes(array):
            return lax.dynamic_slice_in_dim(array.reshape(4, 4, *array.shape[1:]), my_q, 1, axis=1)[:, 0]

        slot_ids = jnp.arange(num_slots, dtype=jnp.int32)
        sum_place = of_my_homes(place.reshape(group_size, num_slots))
        here = (slot_ids // (4 * slots) == my_z) & of_my_homes(member)
        arrives = jnp.where(here, ((slot_ids // slots) % 4 * CAP + sum_place)[:, None, :] + of_my_homes(order), 0)
        hit = of_my_homes(expert_all)[..., None] == slot_expert
        sum_weight = of_my_homes(w_all)

        def plan_of(turn):
            col = jnp.sum(jnp.where(hit & (turn_of == turn), arrives[:, :, None, :], 0), axis=3) - 1
            pad = ((0, 0), (0, 0), (0, 8 - top_k))
            return jnp.concatenate(
                [jnp.pad(col.astype(jnp.float32), pad, constant_values=-1.0), jnp.pad(sum_weight, pad)], axis=2
            )

        shared_out = shared_expert(x_tokens, w1_shared, w3_shared, w2_shared)
        x_all, shared_out = lax.optimization_barrier((x_all, shared_out))
        x_rows = dispatch(x_all, rank_rows, off.reshape(-1), mine.reshape(-1), tail, max_tiles * TM)
        o_send = expert_mlp(
            x_rows, w1_slots, w3_slots, w2_slots, tile_slot, num_tiles, chunk_dst, chunk_count, used, 32 * CAP
        )
        routed = exchange(o_send, plan_of(0), 0, CAP)
        routed = lax.cond(
            crowded, lambda r, o, p: r + exchange(o, p, 1, CAP), lambda r, o, p: r, routed, o_send, plan_of(1)
        )
        return (shared_out + routed).astype(jnp.bfloat16)

    token_spec = P(('dp', 'ep'), None)
    slot_spec = P('ep', None, None)
    return jax.shard_map(device_step, mesh=mesh, in_specs=(token_spec, P(), slot_spec, slot_spec, slot_spec, token_spec, P(), P(), P(), P()), out_specs=token_spec, check_vma=False)
```

```python
import jax
import jax.numpy as jnp
from jax import lax
from jax.experimental import pallas as pl
from jax.experimental.pallas import tpu as pltpu
from jax.sharding import PartitionSpec as P

ROUTE_SCALE = 2.5
TM = 256
WIN = 128
ALIGN = 8
CAP = 384
PIECE = 256
MESH = pl.DeviceIdType.MESH


def gate_weights(x_tokens, assign, slot_expert, w_router):
    num_experts, num_slots = w_router.shape[1], slot_expert.shape[0]
    pick = (jnp.arange(num_experts, dtype=jnp.int32)[:, None] == slot_expert[None, :]).astype(w_router.dtype)
    w_slot = jnp.dot(w_router, pick)
    gate_prob = jax.nn.sigmoid(jnp.dot(x_tokens, w_slot, preferred_element_type=jnp.float32))
    hit = assign[:, :, None] == jnp.arange(num_slots, dtype=jnp.int32)
    picked = jnp.sum(jnp.where(hit, gate_prob[:, None, :], 0.0), axis=2)
    gate_total = jnp.sum(picked, axis=1, keepdims=True)
    return ROUTE_SCALE * picked / jnp.maximum(gate_total, 1e-30)


def shared_expert(x_tokens, w1_shared, w3_shared, w2_shared):
    h_gate = jnp.dot(x_tokens, w1_shared, preferred_element_type=jnp.float32)
    h_up = jnp.dot(x_tokens, w3_shared, preferred_element_type=jnp.float32)
    mid_act = (jax.nn.silu(h_gate) * h_up).astype(jnp.bfloat16)
    return jnp.dot(mid_act, w2_shared, preferred_element_type=jnp.float32)


def dispatch(x_all, rank_rows, off, cpad, tail, max_rows):
    blocks, _, tok = rank_rows.shape
    slots = tail.shape[0]
    dim = x_all.shape[1]

    def kernel(off_ref, cpad_ref, tail_ref, rank_ref, x_ref, out_ref, stage, zeros, sem, zsem):
        b = pl.program_id(0)
        buf = lax.rem(b, 2)

        def copy16(i, src_row, dst_row):
            return pltpu.make_async_copy(
                stage.at[i, pl.ds(pl.multiple_of(src_row, ALIGN), ALIGN), :],
                out_ref.at[pl.ds(pl.multiple_of(dst_row, ALIGN), ALIGN), :],
                sem.at[i],
            )

        def drain(step, i):
            total = cpad_ref[step * slots]
            for s in range(1, slots):
                total = total + cpad_ref[step * slots + s]

            def body(_, c):
                copy16(i, 0, 0).wait()
                return c

            lax.fori_loop(0, lax.div(total, ALIGN), body, 0)

        @pl.when(b >= 2)
        def _():
            drain(b - 2, buf)

        rows = lax.broadcasted_iota(jnp.int32, (WIN, tok), 0)
        sel = [(rows == rank_ref[0, s : s + 1, :]).astype(jnp.float32).astype(jnp.bfloat16) for s in range(slots)]
        win = jnp.dot(jnp.concatenate(sel, axis=0), x_ref[...], preferred_element_type=jnp.float32)
        stage[buf] = win.astype(jnp.bfloat16)
        for s in range(slots):
            start = off_ref[b * slots + s]

            def body(c, carry):
                copy16(buf, s * WIN + c * ALIGN, start + c * ALIGN).start()
                return carry

            lax.fori_loop(0, lax.div(cpad_ref[b * slots + s], ALIGN), body, 0)

        @pl.when(b == blocks - 1)
        def _():
            zeros[...] = jnp.zeros_like(zeros)

            def zcopy(row):
                return pltpu.make_async_copy(zeros, out_ref.at[pl.ds(pl.multiple_of(row, ALIGN), ALIGN), :], zsem)

            for wait in (False, True):
                for s in range(slots):
                    first = off_ref[b * slots + s] + cpad_ref[b * slots + s]

                    def body(c, carry):
                        d = zcopy(first + c * ALIGN)
                        d.wait() if wait else d.start()
                        return carry

                    lax.fori_loop(0, lax.div(tail_ref[s] - first, ALIGN), body, 0)
            drain(b - 1, 1 - buf)
            drain(b, buf)

    return pl.pallas_call(
        kernel,
        grid_spec=pltpu.PrefetchScalarGridSpec(
            num_scalar_prefetch=3,
            grid=(blocks,),
            in_specs=[
                pl.BlockSpec((1, rank_rows.shape[1], tok), lambda b, *_: (b, 0, 0)),
                pl.BlockSpec((tok, dim), lambda b, *_: (b, 0)),
            ],
            out_specs=pl.BlockSpec(memory_space=pl.ANY),
            scratch_shapes=[
                pltpu.VMEM((2, slots * WIN, dim), jnp.bfloat16),
                pltpu.VMEM((ALIGN, dim), jnp.bfloat16),
                pltpu.SemaphoreType.DMA((2,)),
                pltpu.SemaphoreType.DMA,
            ],
        ),
        out_shape=jax.ShapeDtypeStruct((max_rows, dim), jnp.bfloat16),
        compiler_params=pltpu.CompilerParams(vmem_limit_bytes=48 * 2**20),
        name="dispatch",
    )(off, cpad, tail, rank_rows, x_all)


def expert_mlp(x_rows, w1, w3, w2, tile_slot, num_tiles, chunk_dst, chunk_count, used, out_rows):
    dim, ff = w1.shape[1:]
    chunks = TM // ALIGN
    parts = out_rows // CAP

    def kernel(slot_ref, tiles_ref, dst_ref, count_ref, used_ref, x_hbm, w1_hbm, w3_hbm, w2_hbm, o_ref, stage, zeros, w1_buf, w3_buf, w2_buf, step, sem, zsem, wsem):
        tiles = tiles_ref[0]

        def weights(slot):
            k = lax.rem(slot, 2)
            pairs = ((w1_hbm, w1_buf), (w3_hbm, w3_buf), (w2_hbm, w2_buf))
            return [pltpu.make_async_copy(src.at[slot], dst.at[k], wsem.at[k, n]) for n, (src, dst) in enumerate(pairs)]

        for copy in weights(0):
            copy.start()

        def copy16(k, c, row):
            return pltpu.make_async_copy(
                stage.at[k, pl.ds(pl.multiple_of(c * ALIGN, ALIGN), ALIGN), :],
                o_ref.at[pl.ds(pl.multiple_of(row * ALIGN, ALIGN), ALIGN), :],
                sem.at[k],
            )

        def drain(step, k):
            def body(_, carry):
                copy16(k, 0, 0).wait()
                return carry

            lax.fori_loop(0, count_ref[step], body, 0)

        def zero_fill(wait):
            def part(p, carry):
                def body(c, carry):
                    d = pltpu.make_async_copy(
                        zeros, o_ref.at[pl.ds(pl.multiple_of(p * CAP + c * ALIGN, ALIGN), ALIGN), :], zsem
                    )
                    d.wait() if wait else d.start()
                    return carry

                return lax.fori_loop(used_ref[p], CAP // ALIGN, body, carry)

            lax.fori_loop(0, parts, part, 0)

        zeros[...] = jnp.zeros_like(zeros)
        zero_fill(False)
        step[0] = 0

        def tile(x_ref):
            i = step[0]
            step[0] = i + 1
            buf = lax.rem(i, 2)
            slot = slot_ref[i]
            k = lax.rem(slot, 2)

            @pl.when((i == 0) | (slot != slot_ref[jnp.maximum(i - 1, 0)]))
            def _():
                for copy in weights(slot):
                    copy.wait()

                @pl.when(slot + 1 < w1_hbm.shape[0])
                def _():
                    for copy in weights(slot + 1):
                        copy.start()

            @pl.when(i >= 2)
            def _():
                drain(i - 2, buf)

            def multiply(n):
                x = x_ref[0:n, :]
                gate = jnp.dot(x, w1_buf[k], preferred_element_type=jnp.float32)
                up = jnp.dot(x, w3_buf[k], preferred_element_type=jnp.float32)
                mid = (jax.nn.silu(gate) * up).astype(jnp.bfloat16)
                stage[buf, 0:n, :] = jnp.dot(mid, w2_buf[k], preferred_element_type=jnp.float32).astype(jnp.bfloat16)

            half = TM // 2
            pl.when(count_ref[i] * ALIGN <= half)(lambda: multiply(half))
            pl.when(count_ref[i] * ALIGN > half)(lambda: multiply(TM))

            def body(c, carry):
                copy16(buf, c, dst_ref[i * chunks + c]).start()
                return carry

            lax.fori_loop(0, count_ref[i], body, 0)

        pltpu.emit_pipeline(
            tile,
            grid=(tiles,),
            in_specs=[
                pl.BlockSpec((TM, dim), lambda i: (i, 0)),
            ],
        )(x_hbm)

        @pl.when(tiles >= 2)
        def _():
            drain(tiles - 2, lax.rem(tiles, 2))

        drain(tiles - 1, lax.rem(tiles + 1, 2))
        zero_fill(True)

    return pl.pallas_call(
        kernel,
        in_specs=[pl.BlockSpec(memory_space=pltpu.SMEM)] * 5 + [pl.BlockSpec(memory_space=pl.ANY)] * 4,
        out_specs=pl.BlockSpec(memory_space=pl.ANY),
        scratch_shapes=[
            pltpu.VMEM((2, TM, dim), jnp.bfloat16),
            pltpu.VMEM((ALIGN, dim), jnp.bfloat16),
            pltpu.VMEM((2, dim, ff), jnp.bfloat16),
            pltpu.VMEM((2, dim, ff), jnp.bfloat16),
            pltpu.VMEM((2, ff, dim), jnp.bfloat16),
            pltpu.SMEM((1,), jnp.int32),
            pltpu.SemaphoreType.DMA((2,)),
            pltpu.SemaphoreType.DMA,
            pltpu.SemaphoreType.DMA((2, 3)),
        ],
        out_shape=jax.ShapeDtypeStruct((out_rows, dim), jnp.bfloat16),
        compiler_params=pltpu.CompilerParams(vmem_limit_bytes=60 * 2**20),
        name="expert_mlp",
    )(tile_slot, num_tiles.reshape(1), chunk_dst, chunk_count, used, x_rows, w1, w3, w2)


def exchange(o_send, plan, turn, cap):
    dim = o_send.shape[1]
    layers, tok, _ = plan.shape
    pieces = dim // PIECE
    units = layers * pieces
    rows = 4 * cap
    top_k = 6

    def kernel(send_ref, plan_ref, out_ref, recv, zbuf, stage, sel, raw_send, raw_recv, own_sem, z_send, z_recv, out_sem):
        me = lax.axis_index('ep')
        z = me // 4
        q = lax.rem(me, 4)

        def home_of(i):
            low = jnp.where(z == 0, 3 - i, jnp.where(i == 0, 3, jnp.where(i == 1, 0, jnp.where(i == 2, 2, 1))))
            r = 3 - z
            high = jnp.where(r == 0, i, jnp.where(i == 0, 0, jnp.where(i == 1, 3, jnp.where(i == 2, 1, 2))))
            return jnp.where(z < 2, low, high)

        barrier = pltpu.get_barrier_semaphore()
        for d in range(1, 4):
            peer = z * 4 + lax.rem(q + d, 4)
            pl.semaphore_signal(barrier, inc=1, device_id={'ep': peer}, device_id_type=MESH)

        @pl.when(z > 0)
        def _():
            pl.semaphore_signal(barrier, inc=1, device_id={'ep': me - 4}, device_id_type=MESH)

        @pl.when(z < 3)
        def _():
            pl.semaphore_signal(barrier, inc=1, device_id={'ep': me + 4}, device_id_type=MESH)

        pl.semaphore_wait(barrier, 3 + jnp.where(z > 0, 1, 0) + jnp.where(z < 3, 1, 0))

        def block(dst_q, u):
            home, p = home_of(u // pieces), lax.rem(u, pieces)
            row = ((turn * 4 + dst_q) * 4 + home) * CAP
            return send_ref.at[pl.ds(pl.multiple_of(row, 128), cap), pl.ds(pl.multiple_of(p * PIECE, PIECE), PIECE)]

        def raw(d, u):
            dst_q = lax.rem(q + d, 4)
            return pltpu.make_async_remote_copy(
                src_ref=block(dst_q, u),
                dst_ref=recv.at[u, pl.ds(pl.multiple_of(q * cap, cap), cap), :],
                send_sem=raw_send.at[d - 1, u],
                recv_sem=raw_recv.at[d - 1, u],
                device_id={'ep': z * 4 + dst_q},
                device_id_type=MESH,
            )

        def own(u):
            return pltpu.make_async_copy(
                block(q, u), recv.at[u, pl.ds(pl.multiple_of(q * cap, cap), cap), :], own_sem.at[u]
            )

        def start_raw(u, carry):
            for d in range(1, 4):
                raw(d, u).start()
            own(u).start()
            return carry

        lax.fori_loop(0, units, start_raw, 0)

        def up(slot, u):
            return pltpu.make_async_remote_copy(
                src_ref=stage.at[lax.rem(u, 4)],
                dst_ref=zbuf.at[slot, lax.rem(u, pieces)],
                send_sem=z_send.at[lax.rem(u, 4)],
                recv_sem=z_recv.at[slot, lax.rem(u, pieces)],
                device_id={'ep': me + 4},
                device_id_type=MESH,
            )

        def down(slot, u):
            return pltpu.make_async_remote_copy(
                src_ref=stage.at[lax.rem(u, 4)],
                dst_ref=zbuf.at[slot, lax.rem(u, pieces)],
                send_sem=z_send.at[lax.rem(u, 4)],
                recv_sem=z_recv.at[slot, lax.rem(u, pieces)],
                device_id={'ep': me - 4},
                device_id_type=MESH,
            )

        def finish(u):
            p = lax.rem(u, pieces)
            return pltpu.make_async_copy(
                stage.at[lax.rem(u, 4)], out_ref.at[:, pl.ds(pl.multiple_of(p * PIECE, PIECE), PIECE)], out_sem.at[p]
            )

        def unit(u, carry):
            home, p = home_of(u // pieces), lax.rem(u, pieces)
            k = lax.rem(u, 4)

            @pl.when(p == 0)
            def _():
                lanes = lax.broadcasted_iota(jnp.int32, (tok, cap), 1).astype(jnp.float32)
                mine = plan_ref[home]
                for src in range(4):
                    a = jnp.zeros((tok, cap), jnp.float32)
                    for c in range(top_k):
                        a = jnp.where(lanes == mine[:, c : c + 1] - float(src * cap), mine[:, 8 + c : 9 + c], a)
                    hi = a.astype(jnp.bfloat16)
                    rest = a - hi.astype(jnp.float32)
                    mid = rest.astype(jnp.bfloat16)
                    sel[0, :, src * cap : (src + 1) * cap] = hi
                    sel[1, :, src * cap : (src + 1) * cap] = mid
                    sel[2, :, src * cap : (src + 1) * cap] = (rest - mid.astype(jnp.float32)).astype(jnp.bfloat16)

            for d in range(1, 4):
                raw(d, u).wait()
            own(u).wait()

            @pl.when((u >= 4) & (u < units - pieces + 4))
            def _():
                up(0, u - 4).wait_send()

            @pl.when(u >= units - pieces + 4)
            def _():
                finish(u - 4).wait()

            stage[k] = jnp.dot(sel[0], recv[u], preferred_element_type=jnp.float32)

            def term(j, c):
                stage[k] += jnp.dot(sel[j], recv[u], preferred_element_type=jnp.float32)
                return c

            lax.fori_loop(1, 3, term, 0)

            @pl.when(((home < z) & (z < 3)) | ((home >= z) & (z > 0)))
            def _():
                up(home, u).wait_recv()
                stage[k] += zbuf[home, p]

            @pl.when((home == z) & (z < 3))
            def _():
                up(4, u).wait_recv()
                stage[k] += zbuf[4, p]

            @pl.when(home > z)
            def _():
                up(home, u).start()

            @pl.when(home < z)
            def _():
                down(jnp.where(home == z - 1, 4, home), u).start()

            @pl.when(home == z)
            def _():
                finish(u).start()

            return carry

        lax.fori_loop(0, units, unit, 0)
        for u in range(units - 4, units):
            finish(u).wait()

    return pl.pallas_call(
        kernel,
        out_shape=jax.ShapeDtypeStruct((tok, dim), jnp.float32),
        in_specs=[pl.BlockSpec(memory_space=pl.ANY), pl.BlockSpec(memory_space=pltpu.VMEM)],
        out_specs=pl.BlockSpec(memory_space=pl.ANY),
        scratch_shapes=[
            pltpu.VMEM((units, rows, PIECE), jnp.bfloat16),
            pltpu.VMEM((5, pieces, tok, PIECE), jnp.float32),
            pltpu.VMEM((4, tok, PIECE), jnp.float32),
            pltpu.VMEM((3, tok, rows), jnp.bfloat16),
            pltpu.SemaphoreType.DMA((3, units)),
            pltpu.SemaphoreType.DMA((3, units)),
            pltpu.SemaphoreType.DMA((units,)),
            pltpu.SemaphoreType.DMA((4,)),
            pltpu.SemaphoreType.DMA((5, pieces)),
            pltpu.SemaphoreType.DMA((pieces,)),
        ],
        compiler_params=pltpu.CompilerParams(
            collective_id=1 + turn, has_side_effects=True, vmem_limit_bytes=66_000_000
        ),
        name="exchange",
    )(o_send, plan)


def slot_shares(same, counts, slots):
    n = counts.shape[1]

    def kernel(same_ref, count_ref, share_ref):
        same = same_ref[...]
        count = count_ref[...]
        eye = lax.broadcasted_iota(jnp.int32, (n, n), 0) == lax.broadcasted_iota(jnp.int32, (n, n), 1)
        dev = lax.broadcasted_iota(jnp.int32, (n, n), 0) // slots == lax.broadcasted_iota(jnp.int32, (n, n), 1) // slots

        def column(row):
            return jnp.sum(jnp.where(eye, row, 0.0), axis=1, keepdims=True)

        def total(mask, row):
            return jnp.sum(jnp.where(mask, column(row), 0.0), axis=0, keepdims=True)

        one = same > 0.5
        share = 1.0 / total(one, jnp.ones_like(count))
        mean = jnp.sum(share * count) / float(n // slots)

        def step(_, share):
            load = total(dev, share * count)
            share = share * jnp.exp(jnp.clip(1.5 * (1.0 - load / jnp.maximum(mean, 1.0)), -2.0, 2.0))
            share = jnp.maximum(share, 1e-3)
            return share / total(one, share)

        share_ref[...] = lax.fori_loop(0, 24, step, share)

    return pl.pallas_call(
        kernel,
        out_shape=jax.ShapeDtypeStruct((1, n), jnp.float32),
        name="slot_shares",
    )(same, counts)


def place_choices(expert_all, slot_expert, slots):
    tok = expert_all.shape[1]
    num_slots = slot_expert.shape[0]
    wants = jnp.any(expert_all[..., None] == slot_expert, axis=2)
    upto = (jnp.arange(tok)[:, None] >= jnp.arange(tok)[None, :]).astype(jnp.bfloat16)
    order = jnp.einsum('pq,bqs->bps', upto, wants.astype(jnp.bfloat16), preferred_element_type=jnp.float32)
    count = order[:, -1, :]
    same = slot_expert[:, None] == slot_expert[None, :]
    ids = jnp.arange(num_slots)
    earlier = same & (ids[None, :] < ids[:, None])
    copy_no = jnp.sum(earlier, axis=1)
    nxt = same & (copy_no[None, :] == copy_no[:, None] + 1)
    has_next = jnp.any(nxt, axis=1)
    group = jnp.sum(count, axis=0, keepdims=True)
    share = slot_shares(same.astype(jnp.float32), group, slots)

    def bounds(begin):
        lo = jnp.floor(count * begin)
        after = jnp.sum(jnp.where(nxt, begin[:, None, :], 0.0), axis=2)
        return lo, jnp.where(has_next, jnp.floor(count * after), count)

    lo, hi = bounds(jnp.sum(jnp.where(earlier, share, 0.0), axis=1)[None, :])
    even_lo, even_hi = bounds((copy_no / jnp.sum(same, axis=1)).astype(jnp.float32)[None, :])
    over = jnp.max(hi - lo) > 115.0
    lo, hi = jnp.where(over, even_lo, lo), jnp.where(over, even_hi, hi)
    member = wants & (order > lo[:, None, :]) & (order <= hi[:, None, :])
    return member, (order - lo[:, None, :]).astype(jnp.int32), (hi - lo).astype(jnp.int32)


def solution(mesh):
    group_size = mesh.shape['ep']

    def device_step(x_tokens, slot_expert, w1_slots, w3_slots, w2_slots, assign, w_router, w1_shared, w3_shared, w2_shared):
        tok, dim = x_tokens.shape
        top_k = assign.shape[1]
        slots = w1_slots.shape[0]
        num_slots = slots * group_size
        me = lax.axis_index('ep')
        my_z, my_q = me // 4, me % 4
        max_tiles = slots * (group_size * WIN // TM)
        chunks = TM // ALIGN
        weight = gate_weights(x_tokens, assign, slot_expert, w_router)
        x_all = lax.all_gather(x_tokens, 'ep', tiled=True)
        slot_hit = assign[:, :, None] == jnp.arange(num_slots, dtype=jnp.int32)
        expert = jnp.sum(jnp.where(slot_hit, slot_expert + 1, 0), axis=2) - 1
        meta = lax.all_gather(jnp.concatenate([expert.astype(jnp.float32), weight], axis=1), 'ep')
        expert_all = meta[..., :top_k].astype(jnp.int32)
        w_all = meta[..., top_k:]

        def padded(count):
            return (count + ALIGN - 1) // ALIGN * ALIGN

        member, order, count = place_choices(expert_all, slot_expert, slots)
        cpad = padded(count)
        by_dev = cpad.reshape(group_size, group_size, slots)
        crowded = jnp.max(jnp.sum(by_dev, axis=2)) > CAP
        crowded = lax.pmax(crowded.astype(jnp.int32), ('dp', 'ep')) > 0
        split = CAP // WIN
        in_turn = jnp.where(crowded & (jnp.arange(slots) >= split), 1, 0)
        before = jnp.cumsum(by_dev, axis=2) - by_dev
        place = before - jnp.where(in_turn == 1, before[:, :, split : split + 1], 0)
        turn_of = jnp.broadcast_to(in_turn, (group_size, slots)).reshape(num_slots)

        mine = lax.dynamic_slice_in_dim(cpad, me * slots, slots, axis=1)
        my_order = lax.dynamic_slice_in_dim(order, me * slots, slots, axis=2)
        my_member = lax.dynamic_slice_in_dim(member, me * slots, slots, axis=2)
        my_place = lax.dynamic_slice_in_dim(place, me, 1, axis=1)[:, 0]
        home = jnp.arange(group_size, dtype=jnp.int32)
        base = (in_turn[None, :] * 16 + ((home % 4) * 4 + home // 4)[:, None]) * CAP
        tile_ids = jnp.arange(max_tiles, dtype=jnp.int32)
        row0 = jnp.arange(max_tiles * chunks, dtype=jnp.int32) * ALIGN

        tiles = jnp.maximum((jnp.sum(mine, axis=0) + TM - 1) // TM, 1)
        tile_end = jnp.cumsum(tiles)
        off = ((tile_end - tiles) * TM)[None, :] + jnp.cumsum(mine, axis=0) - mine
        num_tiles = jnp.maximum(tile_end[-1], 1)
        tile_slot = jnp.sum((jnp.minimum(tile_ids, num_tiles - 1)[:, None] >= tile_end[None, :-1]).astype(jnp.int32), axis=1)
        tail = jnp.concatenate([tile_end[:-1], num_tiles[None]]) * TM
        rank = jnp.where(my_member, my_order - 1, -1)
        rank_rows = jnp.pad(jnp.transpose(rank, (0, 2, 1)), ((0, 0), (0, 8 - slots), (0, 0)), constant_values=-1)
        lo, hi = off.reshape(-1), (off + mine).reshape(-1)
        inside = (row0[:, None] >= lo[None, :]) & (row0[:, None] < hi[None, :])
        shift = (base + my_place - off).reshape(-1)
        chunk_dst = jnp.sum(jnp.where(inside, shift[None, :] + row0[:, None], 0), axis=1) // ALIGN
        chunk_count = jnp.sum(inside.reshape(max_tiles, chunks, -1).astype(jnp.int32), axis=(1, 2))
        filled = jnp.stack(
            [jnp.sum(jnp.where(in_turn == 0, mine, 0), axis=1), jnp.where(crowded, jnp.sum(jnp.where(in_turn == 1, mine, 0), axis=1), CAP)]
        )
        used = jnp.transpose(filled.reshape(2, 4, 4), (0, 2, 1)).reshape(-1) // ALIGN

        def of_my_homes(array):
            return lax.dynamic_slice_in_dim(array.reshape(4, 4, *array.shape[1:]), my_q, 1, axis=1)[:, 0]

        slot_ids = jnp.arange(num_slots, dtype=jnp.int32)
        sum_place = of_my_homes(place.reshape(group_size, num_slots))
        here = (slot_ids // (4 * slots) == my_z) & of_my_homes(member)
        arrives = jnp.where(here, ((slot_ids // slots) % 4 * CAP + sum_place)[:, None, :] + of_my_homes(order), 0)
        hit = of_my_homes(expert_all)[..., None] == slot_expert
        sum_weight = of_my_homes(w_all)

        def plan_of(turn):
            col = jnp.sum(jnp.where(hit & (turn_of == turn), arrives[:, :, None, :], 0), axis=3) - 1
            pad = ((0, 0), (0, 0), (0, 8 - top_k))
            return jnp.concatenate(
                [jnp.pad(col.astype(jnp.float32), pad, constant_values=-1.0), jnp.pad(sum_weight, pad)], axis=2
            )

        shared_out = shared_expert(x_tokens, w1_shared, w3_shared, w2_shared)
        x_all, shared_out = lax.optimization_barrier((x_all, shared_out))
        x_rows = dispatch(x_all, rank_rows, off.reshape(-1), mine.reshape(-1), tail, max_tiles * TM)
        o_send = expert_mlp(
            x_rows, w1_slots, w3_slots, w2_slots, tile_slot, num_tiles, chunk_dst, chunk_count, used, 32 * CAP
        )
        routed = exchange(o_send, plan_of(0), 0, CAP)
        routed = lax.cond(
            crowded, lambda r, o, p: r + exchange(o, p, 1, CAP), lambda r, o, p: r, routed, o_send, plan_of(1)
        )
        return (shared_out + routed).astype(jnp.bfloat16)

    token_spec = P(('dp', 'ep'), None)
    slot_spec = P('ep', None, None)
    return jax.shard_map(device_step, mesh=mesh, in_specs=(token_spec, P(), slot_spec, slot_spec, slot_spec, token_spec, P(), P(), P(), P()), out_specs=token_spec, check_vma=False)
```
